32 devices in a mesh: ep: 8 (over z, y), dp: 4 (over x, core).
Axes of the slice: x: 2, y: 2, z: 4, core: 2. Of those that a mesh axis runs over, the one named last changes fastest.
Arguments:
- tokens: bfloat16 [4096, 7168], P(('dp', 'ep')), parts along dimension 0, may hold values from -18 to 18
- expert_ids: int32 [4096, 2], P(('dp', 'ep')), parts along dimension 0, may hold values from 0 to 3, all different within a row; in each aligned block of 128 rows (0 to 127, 128 to 255, ...) at most 128 rows name the same one
- affinity: float32 [4096, 2], P(('dp', 'ep')), parts along dimension 0, may hold values from 0.05 to 1
- w_gate: bfloat16 [8, 7168, 512], P('ep'), may hold values from -0.0625 to 0.0625
- w_up: bfloat16 [8, 7168, 512], P('ep'), may hold values from -0.0625 to 0.0625
- w_down: bfloat16 [8, 512, 7168], P('ep'), may hold values from -0.1875 to 0.1875
Outputs:
- mixed: bfloat16 [4096, 7168], P(('dp', 'ep')), parts along dimension 0
The draws below stay inside these ranges and needn't reach their ends.
There are 4 independent parts, one for each index of `dp`. The reference program is written for one: setup_inputs(seed, part) draws one part's arguments, and reference() takes and returns one part's arrays. A program takes and returns all parts, laid end to end along the dimension named above; an argument that names none is the same for every part. Nothing has to cross between parts.
Inputs may be any that keep to these rules, and one draw needn't show every extreme that they name: `expert_ids`: each row names 2 different experts; among the rows of one index of ep no expert is named by more than 128 rows.
All inputs are finite; a program needn't handle non-finite values.
Results may differ from the reference program's by a relative error of at most 0.019.
Values may be sent and summed in bfloat16 or wider, within the bound.
A program may use at most 256 MiB of HBM per device.

```python
import math
import jax
import jax.numpy as jnp
import numpy as np
from jax import lax

D = 7168
FF = 1024
TOP = 2
TOK_DEV = 128
FF_HALF = 512
EXPERTS = 4
CAP = 128
TOKENS = 1024
N_EP = 8


def draw_tokens(key, part):
    scale_key, block_key, value_key = jax.random.split(key, 3)
    row_scale = jnp.exp(jax.random.uniform(scale_key, (TOKENS, 1, 1), jnp.float32, jnp.log(0.8), jnp.log(1.25)))
    block_scale = jnp.exp(jax.random.uniform(block_key, (TOKENS, D // 16, 1), jnp.float32, jnp.log(0.05), jnp.log(2.0)))
    values = jnp.clip(jax.random.normal(value_key, (TOKENS, D // 16, 16), jnp.float32), -5.0, 5.0)
    return (values * block_scale * row_scale).reshape(TOKENS, D).astype(jnp.bfloat16)


def block_levels(own_key, shape, cuts, least, high):
    def one(dim, blocks):
        steps = jax.random.uniform(jax.random.fold_in(jax.random.fold_in(own_key, 6), dim), (blocks,), jnp.float32, least / len(cuts), high / len(cuts))
        return jnp.repeat(jnp.exp(steps), shape[dim] // blocks).reshape((-1,) + (1,) * (len(shape) - dim - 1))

    gain = one(*cuts[0])
    for cut in cuts[1:]:
        gain = gain * one(*cut)
    return gain


def deal_out(stream_key, own, number, rows, count, top, most, slope):
    ranking = jax.random.permutation(stream_key, count)
    crowded, usual = load_shares(count, rows * top, most, slope, True), load_shares(count, rows * top, most, slope, False)
    places = jnp.arange(count)

    def named(lengths, rotation):
        used = int((lengths > 0).sum())
        fixed = max(1, used // 4)
        passed = fixed + (places - fixed + rotation * (used - fixed)) % max(1, count - fixed)
        return jnp.zeros((count,), jnp.int32).at[ranking[jnp.where(places < fixed, places, passed)]].set(jnp.asarray(lengths, jnp.int32))

    lengths = jnp.where(number % 4 == 0, named(crowded, number // 4), named(usual, number - number // 4 - 1))
    mixed = jax.random.permutation(jax.random.fold_in(own, 3), count)
    donor, sink = mixed[0:count // 2 * 2:2], mixed[1:count // 2 * 2:2]
    room = jnp.minimum(lengths[donor] - 1, most - lengths[sink]) // 2
    room = jnp.where((donor == ranking[0]) | (sink == ranking[0]) | (lengths[sink] == 0), 0, jnp.maximum(room, 0))
    passed = jax.random.randint(jax.random.fold_in(own, 4), (count // 2,), 0, 1 << 20) % (room + 1)
    lengths = lengths.at[donor].add(-passed).at[sink].add(passed)
    labels = jnp.searchsorted(jnp.cumsum(lengths), jnp.arange(rows * top), side="right").astype(jnp.int32)
    grid = labels.reshape(top, rows).T
    grid = grid[jax.random.permutation(jax.random.fold_in(own, 1), rows)]
    rotation = jax.random.randint(jax.random.fold_in(own, 2), (rows, 1), 0, top)
    return jnp.take_along_axis(grid, (jnp.arange(top)[None, :] + rotation) % top, axis=1)


def load_shares(number_of, total, bound, lean, full):
    weights = [(1 << 20) // math.isqrt(standing ** lean) + 1 for standing in range(1, number_of + 1)]
    largest = bound if full else min(bound, max(-(-total // number_of), total * weights[0] // sum(weights)))
    least = 1 if total - largest >= number_of - 1 else 0
    counts, rest = [largest] + [least] * (number_of - 1), total - largest - least * (number_of - 1)
    while rest > 0:
        candidates = [i for i in range(1, number_of) if counts[i] < largest] or [i for i in range(1, number_of) if counts[i] < bound]
        mass, budget = sum([weights[i] for i in candidates]), rest
        for i in candidates:
            more = min(bound - counts[i], max(1, budget * weights[i] // mass), rest)
            counts[i] = counts[i] + more
            rest = rest - more
    return np.array(counts)


def noise(rng, extent, deviation, reach, cuts=(), kind=jnp.bfloat16):
    values = jax.random.normal(rng, extent, jnp.float32) * deviation
    if len(cuts) > 0:
        values = block_levels(rng, extent, cuts, -0.22, 0.18) * values
    return jnp.clip(values, min=-reach, max=reach).astype(kind)


def setup_inputs(seed: int = 0, part: int = 0) -> dict:
    streams_of = jax.random.split(jax.random.key(seed), 7)
    own_keys = jax.random.split(jax.random.fold_in(streams_of[6], part), 7)
    tokens = draw_tokens(jax.random.fold_in(jax.random.fold_in(streams_of[6], part), 71), part)
    expert_ids_keys = jax.random.split(jax.random.fold_in(own_keys[1], 1), TOKENS // TOK_DEV)
    expert_ids_turns = jax.random.permutation(jax.random.fold_in(own_keys[1], 3), TOKENS // TOK_DEV)
    expert_ids = jax.vmap(lambda own, number: deal_out(jax.random.fold_in(own_keys[1], 2), own, number, TOK_DEV, EXPERTS, TOP, CAP, 3))(expert_ids_keys, expert_ids_turns).reshape((TOKENS, TOP))
    affinity = jnp.clip(jnp.exp(math.log(1.0) - 2.9957323 * jax.random.uniform(own_keys[2], (TOKENS, TOP), jnp.float32) ** block_levels(own_keys[2], (TOKENS, TOP), ((0, 8),), -0.2, 0.2)), 0.05, 1.0)
    w_gate = noise(streams_of[3], (N_EP, D, FF_HALF), D ** -0.5, 0.0625, ((0, 8),))
    w_up = noise(streams_of[4], (N_EP, D, FF_HALF), D ** -0.5, 0.0625, ((0, 8),))
    w_down = noise(streams_of[5], (N_EP, FF_HALF, D), FF ** -0.5, 0.1875, ((0, 8),))
    return {"tokens": tokens, "expert_ids": expert_ids, "affinity": affinity, "w_gate": w_gate, "w_up": w_up, "w_down": w_down}


def quantize(tokens):
    count_rows = tokens.shape[0]
    blocks = tokens.astype(jnp.float32).reshape(count_rows, -1, 16)
    largest = jnp.max(jnp.abs(blocks), axis=2)
    scales = (jnp.maximum(largest, 0.25) / 9.0).astype(jnp.bfloat16)
    divided = blocks / scales.astype(jnp.float32)[:, :, None]
    payload = jnp.clip(divided, -6.0, 6.0).astype(jnp.bfloat16).reshape(count_rows, -1)
    return payload, scales


def restore(payload, scales):
    count_rows = payload.shape[0]
    values = payload.astype(jnp.float32).reshape(count_rows, -1, 16) * scales.astype(jnp.float32)[:, :, None]
    return values.astype(jnp.bfloat16).reshape(count_rows, -1)


def half_expert(restored, gate_half, up_half, down_half):
    gate = jnp.dot(restored, gate_half, preferred_element_type=jnp.float32)
    upward = jnp.dot(restored, up_half, preferred_element_type=jnp.float32)
    hidden = (jax.nn.silu(gate) * upward).astype(jnp.bfloat16)
    return jnp.dot(hidden, down_half, preferred_element_type=jnp.float32).astype(jnp.bfloat16)


def reference(tokens, expert_ids, affinity, w_gate, w_up, w_down):
    payload, scales = quantize(tokens)
    restored = restore(payload, scales)
    flat_ids = expert_ids.reshape(-1).astype(jnp.int32)
    assigned = flat_ids.shape[0]
    slot_total = N_EP * CAP

    def per_expert(expert):
        others = (flat_ids != expert).astype(jnp.int32)
        ordering = jnp.argsort(others, stable=True)[:slot_total].astype(jnp.int32)
        picked = restored[ordering // TOP]
        first_half = half_expert(picked, w_gate[2 * expert], w_up[2 * expert], w_down[2 * expert])
        second_half = half_expert(picked, w_gate[2 * expert + 1], w_up[2 * expert + 1], w_down[2 * expert + 1])
        summed = (first_half.astype(jnp.float32) + second_half.astype(jnp.float32)).astype(jnp.bfloat16)
        count_live = jnp.sum(1 - others)
        target_rows = jnp.where(jnp.arange(slot_total, dtype=jnp.int32) < count_live, ordering, assigned).astype(jnp.int32)
        return summed, target_rows

    outputs, targets = lax.map(per_expert, jnp.arange(EXPERTS, dtype=jnp.int32))
    per_slot = jnp.zeros((assigned, D), jnp.bfloat16).at[targets.reshape(-1)].set(outputs.reshape(-1, D), mode="drop")
    weights = affinity / jnp.sum(affinity, axis=1, keepdims=True)
    combined = jnp.sum(weights[:, :, None] * per_slot.astype(jnp.float32).reshape(TOKENS, TOP, D), axis=1)
    return combined.astype(jnp.bfloat16)
```

```python
import collections
import functools

import jax
import jax.numpy as jnp
from jax import lax
from jax.experimental import pallas as pl
from jax.experimental.pallas import tpu as pltpu
from jax.sharding import PartitionSpec as P

LINE = 4
LANES = 128
MESH = pl.DeviceIdType.MESH
VMEM_LIMIT = 67_000_000
GROUPS = 2
CHUNKS = 4
PARTS = 7
DOWN = 2
PER = CHUNKS // GROUPS
STEPS = LINE * GROUPS
ORDERS = ((3, 2, 1, 0), (3, 0, 2, 1), (0, 3, 1, 2), (0, 1, 2, 3))


def requantized(tokens):
    rows, width = tokens.shape
    blocks = tokens.astype(jnp.float32).reshape(rows, -1, 16)
    largest = jnp.max(jnp.abs(blocks), axis=2)
    scales = (jnp.maximum(largest, 0.25) / 9.0).astype(jnp.bfloat16).astype(jnp.float32)
    divided = blocks / scales[:, :, None]
    payload = jnp.clip(divided, -6.0, 6.0).astype(jnp.bfloat16).astype(jnp.float32)
    return (payload * scales[:, :, None]).astype(jnp.bfloat16).reshape(rows, width)


def swap(values, lane, distance):
    high = (lane // distance) % 2 == 1
    width = values.shape[1]
    return jnp.where(
        high, pltpu.roll(values, distance, 1), pltpu.roll(values, width - distance, 1)
    )


def quantize_at(ref):
    width = ref.shape[1]

    def body(i, carry):
        at = pl.ds(pl.multiple_of(i * LANES, LANES), LANES)
        values = ref[:, at].astype(jnp.float32)
        lane = lax.broadcasted_iota(jnp.int32, values.shape, 1)
        largest = jnp.abs(values)
        for distance in (1, 2, 4, 8):
            largest = jnp.maximum(largest, swap(largest, lane, distance))
        scales = (jnp.maximum(largest, 0.25) / 9.0).astype(jnp.bfloat16).astype(jnp.float32)
        payload = jnp.clip(values / scales, -6.0, 6.0).astype(jnp.bfloat16).astype(jnp.float32)
        ref[:, at] = (payload * scales).astype(ref.dtype)
        return carry

    lax.fori_loop(0, width // LANES, body, 0)


def down_line():
    ready = {z: {(z, c): 0 for c in range(CHUNKS)} for z in range(LINE)}
    sends = {z: [] for z in range(LINE)}
    for slot in range(8 * CHUNKS):
        for z in range(LINE - 1, 0, -1):
            able = [key for key, when in ready[z].items() if when <= slot]
            if able:
                owner, c = min(able, key=lambda key: (-key[0], key[1]))
                del ready[z][owner, c]
                sends[z].append((slot, owner, c))
                if z - 1 > 0:
                    ready[z - 1][owner, c] = slot + 1
    return sends


FIRST, START = -1, 0


def before(k):
    return 1 + 3 * k


def middle(k):
    return 2 + 3 * k


def after(k):
    return 3 + 3 * k


LAST = after(STEPS)


def script(z):
    last = LINE - 1
    down = down_line()
    up = {p: [(slot, last - o, c) for slot, o, c in down[last - p]] for p in range(LINE)}
    moves = [(slot, "down", o, c) for slot, o, c in down[z]]
    moves += [(slot, "up", o, c) for slot, o, c in up[z]]
    arrival = {(z, c): 0 for c in range(CHUNKS)}
    if z < last:
        arrival.update({(o, c): slot + 1 for slot, o, c in down[z + 1]})
    if z > 0:
        arrival.update({(o, c): slot + 1 for slot, o, c in up[z - 1]})
    steps = [(ORDERS[z][k // GROUPS], k % GROUPS) for k in range(STEPS)]
    chunks = [[(o, g * PER + i) for i in range(PER)] for o, g in steps]
    opening = CHUNKS + PER
    raw = []

    def add(place, rank, op):
        raw.append((place, rank, len(raw), op))

    for slot, way, o, c in moves:
        if slot == 0:
            add(FIRST, slot, ("line", way, o, c))
        elif slot <= opening:
            add(START, slot, ("line", way, o, c))
        else:
            add(after((slot - opening - 1) // PER), slot, ("line", way, o, c))
    for i in range(DOWN):
        add(FIRST, 1, ("weights", i))
        add(START, (i + 1) * CHUNKS / DOWN + 0.6, ("weights y", i))
    add(START, CHUNKS / DOWN * 2 + 1.1, ("weights x", 0))
    for i in range(1, DOWN):
        add(START if i < DOWN - 1 else before(0), 99, ("weights x", i))
    latest = 0
    for o, c in chunks[0] + chunks[1][:1]:
        latest = max(latest, arrival[o, c] + 0.2)
        add(START, latest, ("cross", o, c))
    for k in range(STEPS):
        o, g = steps[k]
        for o, c in chunks[k]:
            add(before(k), 0, ("arrived", o, c))
            add(before(k), 1, ("crossed", o, c))
            add(middle(k), 2, ("free", o, c))
        if k + 1 < STEPS:
            for o, c in chunks[k + 1][1:]:
                add(middle(k), 0, ("cross", o, c))
        if k + 2 < STEPS:
            add(after(k), -1, ("cross",) + chunks[k + 2][0])
    if 0 < z < last:
        far, back, near = ORDERS[z][:3]
        for k, o, g in (
            (1, far, 0),
            (2, far, 1),
            (3, back, 0),
            (4, back, 1),
            (4, near, 0),
            (5, near, 1),
        ):
            add(after(k), 99, ("add", o, g))
    for g in range(GROUPS):
        add(after(STEPS - GROUPS + g), 100, ("finish", g))
    waited, sent, freed = set(), set(), set()
    done = collections.defaultdict(list)
    for place, rank, number, op in sorted(raw):
        out = done[place]
        if op[0] in ("line", "cross", "arrived"):
            key = op[-2:]
            if key[0] != z and key not in waited:
                waited.add(key)
                out.append(("wait",) + key)
        if op[0] == "arrived":
            continue
        if op[0] in ("line", "cross"):
            assert op[-2:] not in freed
            sent.add((op[1] if op[0] == "line" else "cross",) + op[-2:])
        if op[0] == "free":
            freed.add(op[-2:])
            for way in ("up", "down", "cross"):
                if (way,) + op[-2:] in sent:
                    out.append(("sent", way) + op[-2:])
            continue
        out.append(op)
    assert len(freed) == LINE * CHUNKS
    return done


def layer(
    tokens_ref,
    share_ref,
    gate_ref,
    up_ref,
    down_ref,
    out_ref,
    x_ref,
    wg_ref,
    wu_ref,
    wd_ref,
    hid_ref,
    peer_ref,
    got_ref,
    shares_ref,
    local,
    line_send,
    line_recv,
    cross_send,
    cross_recv,
    hid_send,
    hid_recv,
    part_send,
    part_recv,
    share_send,
    share_recv,
    w_send,
    w_recv,
):
    me, dp = lax.axis_index("ep"), lax.axis_index("dp")
    here, y = me // 2, lax.rem(me, 2)
    other = 1 - y
    last = LINE - 1
    peer = {"ep": 2 * here + other}
    twin = {"dp": dp + 1 - 2 * lax.rem(dp, 2)}
    across = {"dp": lax.rem(dp + 2, 4)}
    rows, width = out_ref.shape
    lot = rows // GROUPS
    size = rows // CHUNKS
    part = width // PARTS
    inner = wg_ref.shape[1]
    scripts = [script(z) for z in range(LINE)]

    def chunk(o, c):
        g, i = c // PER, c % PER
        return x_ref.at[o, g, pl.ds(pl.multiple_of(y * lot + i * size, size), size), :]

    def crossing(o, c):
        g, i = c // PER, c % PER
        return x_ref.at[o, g, pl.ds(pl.multiple_of(other * lot + i * size, size), size), :]

    def remote(source, place, send, recv, target):
        return pltpu.make_async_remote_copy(
            src_ref=source,
            dst_ref=place,
            send_sem=send,
            recv_sem=recv,
            device_id=target,
            device_id_type=MESH,
        )

    def line(way, o, c):
        target = {"ep": me + 2 if way == "up" else me - 2}
        place = chunk(o, c)
        return remote(
            place, place, line_send.at[0 if way == "up" else 1, o, c], line_recv.at[o, c], target
        )

    def cross(o, c):
        place = chunk(o, c)
        return remote(place, place, cross_send.at[o, c], cross_recv.at[o, c], peer)

    quarter = down_ref.shape[1] // 4
    piece = quarter // DOWN

    def rows_of(q, i):
        return pl.ds(pl.multiple_of(q * quarter + i * piece, piece), piece)

    def weight(kind, half, q, i, target):
        place = wd_ref.at[half, rows_of(q, i), :]
        source = down_ref.at[0, rows_of(q, i), :] if kind == 0 else place
        return remote(source, place, w_send.at[kind, i], w_recv.at[kind, i], target)

    q_mine, q_across = dp, lax.rem(dp + 2, 4)
    twin_dp = dp + 1 - 2 * lax.rem(dp, 2)
    q_twin, q_twin_across = twin_dp, lax.rem(twin_dp + 2, 4)

    def partial(z, o, g, n, way):
        step = 1 if way == "up" else -1
        nearest = isinstance(z, int) and z + step == o
        slot = LINE if way == "down" and nearest else o
        return part_copy(o, slot, g, n, {"ep": me + 2 * step})

    def part_copy(o, slot, g, n, target):
        columns = pl.ds(pl.multiple_of(n * part, part), part)
        source = x_ref.at[o, g, pl.ds(pl.multiple_of(y * lot, lot), lot), columns]
        return remote(
            source,
            got_ref.at[slot, g, :, columns],
            part_send.at[o, g, n],
            part_recv.at[slot, g, n],
            target,
        )

    def got_wait(slot, g, n):
        columns = pl.ds(pl.multiple_of(n * part, part), part)
        place = got_ref.at[slot, g, :, columns]
        remote(place, place, part_send.at[0, g, n], part_recv.at[slot, g, n], peer).wait_recv()

    def sum_into(target, at, sources):
        step = 16

        def body(i, carry):
            lines = pl.ds(pl.multiple_of(i * step, step), step)
            total = sources[0][lines, at].astype(jnp.float32)
            for source in sources[1:]:
                total = total + source[lines, at].astype(jnp.float32)
            target[lines, at] = total.astype(target.dtype)
            return carry

        lax.fori_loop(0, lot // step, body, 0)

    def run(z, op):
        kind = op[0]
        if kind == "wait":
            line("up", *op[1:]).wait_recv()
        elif kind == "line":
            line(*op[1:]).start()
        elif kind == "cross":
            cross(*op[1:]).start()
        elif kind == "crossed":
            place = crossing(*op[1:])
            o, c = op[1:]
            remote(place, place, cross_send.at[o, c], cross_recv.at[o, c], peer).wait_recv()
        elif kind == "sent":
            way, o, c = op[1:]
            (cross(o, c) if way == "cross" else line(way, o, c)).wait_send()
        elif kind == "weights":
            weight(0, y, q_mine, op[1], peer).start()
        elif kind == "weights y":
            weight(0, other, q_mine, op[1], peer).wait_recv()
            weight(1, other, q_mine, op[1], across).start()
            weight(2, other, q_mine, op[1], twin).start()
        elif kind == "weights x":
            weight(1, other, q_across, op[1], across).wait_recv()
            weight(3, other, q_across, op[1], twin).start()
        elif kind == "add":
            o, g = op[1:]
            mine = x_ref.at[o, g, pl.ds(pl.multiple_of(y * lot, lot), lot), :]

            def body(n, carry):
                got_wait(o, g, n)
                at = pl.ds(pl.multiple_of(n * part, part), part)
                sum_into(mine, at, [mine, got_ref.at[o, g]])
                partial(z, o, g, n, "up" if o > z else "down").start()
                return carry

            lax.fori_loop(0, PARTS, body, 0)
        elif kind == "finish":
            g = op[1]
            mine = x_ref.at[z, g, pl.ds(pl.multiple_of(y * lot, lot), lot), :]
            slots = ([z] if z > 0 else []) + ([LINE] if z < last else [])

            def body(n, carry):
                for slot in slots:
                    got_wait(slot, g, n)
                at = pl.ds(pl.multiple_of(n * part, part), part)
                sum_into(
                    out_ref.at[pl.ds(g * lot, lot), :],
                    at,
                    [mine] + [got_ref.at[slot, g] for slot in slots],
                )
                return carry

            lax.fori_loop(0, PARTS, body, 0)
        else:
            raise ValueError(kind)

    def play(place):
        for z in range(LINE):
            ops = scripts[z][place]
            if ops:

                @pl.when(here == z)
                def _(z=z, ops=ops):
                    for op in ops:
                        run(z, op)

    def play_in(kind, k):
        for z in range(LINE):

            @pl.when(here == z)
            def _(z=z):
                for step in range(STEPS):
                    ops = scripts[z][kind(step)]
                    if ops:

                        @pl.when(k == step)
                        def _(ops=ops):
                            for op in ops:
                                run(z, op)

    own_rows = pl.ds(pl.multiple_of(y * lot, lot), lot)
    loads = []

    def load(source, place):
        copy = pltpu.make_async_copy(source, place, local.at[len(loads)])
        loads.append(copy)
        copy.start()

    for g in range(GROUPS):
        load(tokens_ref.at[pl.ds(g * lot, lot), :], x_ref.at[here, g, own_rows, :])
    load(gate_ref.at[0], wg_ref)
    load(up_ref.at[0], wu_ref)
    load(down_ref.at[0], wd_ref.at[y])
    barrier = pltpu.get_barrier_semaphore()
    targets = [{"ep": lax.rem(me + 2 * step, 2 * LINE)} for step in range(1, LINE)]
    targets += [peer, twin, across]
    for target in targets:
        pl.semaphore_signal(barrier, inc=1, device_id=target, device_id_type=MESH)

    def quantize(c):
        g, i = c // PER, c % PER
        if i == 0:
            loads[g].wait()
        quantize_at(chunk(here, c))

    quantize(0)
    pl.semaphore_wait(barrier, len(targets))
    play(FIRST)
    shares = []
    for step in range(1, LINE):
        target = {"ep": lax.rem(me + 2 * step, 2 * LINE)}
        copy = remote(
            share_ref, shares_ref.at[here], share_send.at[step], share_recv.at[step], target
        )
        copy.start()
        shares.append(copy)
    shares_ref[here] = share_ref[...]
    for c in range(1, CHUNKS):
        quantize(c)
    play(START)
    for copy in loads[GROUPS:]:
        copy.wait()
    for copy in shares:
        copy.wait()

    def order(k):
        b = k // GROUPS
        value = jnp.int32(0)
        for z in range(LINE):
            for i in range(LINE):
                value = jnp.where((here == z) & (b == i), ORDERS[z][i], value)
        return value

    half = inner // 2

    def step_of(k, carry):
        o, g = order(k), lax.rem(k, GROUPS)
        play_in(before, k)

        def hidden(j, c):
            at = pl.ds(pl.multiple_of(j * half, half), half)
            x = x_ref[o, g]
            gate = jnp.dot(x, wg_ref[:, at], preferred_element_type=jnp.float32)
            upward = jnp.dot(x, wu_ref[:, at], preferred_element_type=jnp.float32)
            hid_ref[o, g, :, at] = (jax.nn.silu(gate) * upward).astype(hid_ref.dtype)
            return c

        lax.fori_loop(0, 2, hidden, 0)
        other_rows = pl.ds(pl.multiple_of(other * lot, lot), lot)
        back = remote(
            hid_ref.at[o, g, other_rows, :],
            peer_ref.at[o, g],
            hid_send.at[o, g],
            hid_recv.at[o, g],
            peer,
        )
        back.start()
        play_in(middle, k)

        @pl.when(k == 0)
        def _():
            for i in range(DOWN):
                weight(2, other, q_twin, i, twin).wait_recv()
                weight(3, other, q_twin_across, i, twin).wait_recv()

        back.wait()
        row = shares_ref[o, pl.ds(here, 1), :]
        square = (lot, row.shape[1])
        lane = lax.broadcasted_iota(jnp.int32, square, 1)
        line_of = lax.broadcasted_iota(jnp.int32, square, 0)
        share = jnp.sum(
            jnp.where(lane == line_of + g * lot, jnp.broadcast_to(row, square), 0.0),
            axis=1,
            keepdims=True,
        )
        begins = ((here == 0) & (o != 0)) | ((here == last) & (o != last))
        slot = jnp.where((here == last) & (o == last - 1), LINE, o)
        onward = jnp.where(here == 0, me + 2, me - 2)

        def down(n, c):
            at = pl.ds(pl.multiple_of(n * part, part), part)
            total = jnp.dot(
                hid_ref[o, g, own_rows, :], wd_ref[y, :, at], preferred_element_type=jnp.float32
            ) + jnp.dot(peer_ref[o, g], wd_ref[other, :, at], preferred_element_type=jnp.float32)
            x_ref[o, g, own_rows, at] = (total * share).astype(x_ref.dtype)

            @pl.when(begins)
            def _():
                part_copy(o, slot, g, n, {"ep": onward}).start()

            return c

        lax.fori_loop(0, PARTS, down, 0)
        play_in(after, k)
        return carry

    lax.fori_loop(0, STEPS, step_of, 0)

    def drain(i, carry):
        o, g = i // GROUPS, lax.rem(i, GROUPS)

        @pl.when(o != here)
        def _():
            def body(n, c):
                part_copy(o, o, g, n, peer).wait_send()
                return c

            lax.fori_loop(0, PARTS, body, 0)

        return carry

    lax.fori_loop(0, STEPS, drain, 0)
    for i in range(DOWN):
        weight(0, y, q_mine, i, peer).wait_send()
        weight(1, other, q_mine, i, across).wait_send()
        weight(2, other, q_mine, i, twin).wait_send()
        weight(3, other, q_across, i, twin).wait_send()


def fused(tokens, share, w_gate, w_up, w_down):
    rows, width = tokens.shape
    inner = w_gate.shape[2]
    lot = rows // GROUPS
    kind = tokens.dtype
    dma = pltpu.SemaphoreType.DMA
    anywhere = pl.BlockSpec(memory_space=pl.ANY)
    inside = pl.BlockSpec(memory_space=pltpu.VMEM)
    return pl.pallas_call(
        layer,
        out_shape=jax.ShapeDtypeStruct((rows, width), kind),
        in_specs=[anywhere, inside, anywhere, anywhere, anywhere],
        out_specs=inside,
        scratch_shapes=[
            pltpu.VMEM((LINE, GROUPS, 2 * lot, width), kind),
            pltpu.VMEM((width, inner), kind),
            pltpu.VMEM((width, inner), kind),
            pltpu.VMEM((2, inner, width), kind),
            pltpu.VMEM((LINE, GROUPS, 2 * lot, inner), kind),
            pltpu.VMEM((LINE, GROUPS, lot, inner), kind),
            pltpu.VMEM((LINE + 1, GROUPS, lot, width), kind),
            pltpu.VMEM((LINE,) + share.shape, share.dtype),
            dma((GROUPS + 3,)),
            dma((2, LINE, CHUNKS)),
            dma((LINE, CHUNKS)),
            dma((LINE, CHUNKS)),
            dma((LINE, CHUNKS)),
            dma((LINE, GROUPS)),
            dma((LINE, GROUPS)),
            dma((LINE, GROUPS, PARTS)),
            dma((LINE + 1, GROUPS, PARTS)),
            dma((LINE,)),
            dma((LINE,)),
            dma((4, DOWN)),
            dma((4, DOWN)),
        ],
        compiler_params=pltpu.CompilerParams(
            collective_id=0, has_side_effects=True, vmem_limit_bytes=VMEM_LIMIT
        ),
        name="layer",
    )(tokens, share, w_gate, w_up, w_down)


def on_device(tokens, expert_ids, affinity, w_gate, w_up, w_down):
    n = lax.axis_size("ep")
    experts = n // 2
    own = lax.axis_index("ep") // 2
    rows, width = tokens.shape
    weights = affinity / jnp.sum(affinity, axis=1, keepdims=True)
    padded = -(-experts // 8) * 8
    names = jnp.arange(padded, dtype=jnp.int32)[:, None]
    shares = sum(
        jnp.where(expert_ids[:, k][None, :] == names, weights[:, k][None, :], 0.0)
        for k in range(weights.shape[1])
    )
    by_line = (
        experts == LINE
        and lax.axis_size("dp") == 4
        and rows == LANES
        and width % (PARTS * LANES) == 0
    )
    if by_line:
        return fused(tokens, shares, w_gate, w_up, w_down)
    every = lax.all_gather(requantized(tokens), "ep", axis=0, tiled=False)
    shares = lax.all_gather(shares, "ep", axis=0, tiled=False)
    every = every.reshape(n * rows, width)
    share = lax.dynamic_slice_in_dim(shares, own, 1, axis=1).reshape(n * rows, 1)
    gate = jnp.dot(every, w_gate[0], preferred_element_type=jnp.float32)
    upward = jnp.dot(every, w_up[0], preferred_element_type=jnp.float32)
    hidden = (jax.nn.silu(gate) * upward).astype(jnp.bfloat16)
    partial = jnp.dot(hidden, w_down[0], preferred_element_type=jnp.float32)
    scaled = (partial * share).astype(jnp.bfloat16)
    return lax.psum_scatter(scaled, "ep", scatter_dimension=0, tiled=True)


def solution(mesh):
    in_specs = (
        P(("dp", "ep"), None),
        P(("dp", "ep"), None),
        P(("dp", "ep"), None),
        P("ep", None, None),
        P("ep", None, None),
        P("ep", None, None),
    )
    return jax.shard_map(
        on_device, mesh=mesh, in_specs=in_specs, out_specs=P(("dp", "ep"), None), check_vma=False
    )
```

```python
import collections
import functools

import jax
import jax.numpy as jnp
from jax import lax
from jax.experimental import pallas as pl
from jax.experimental.pallas import tpu as pltpu
from jax.sharding import PartitionSpec as P

LINE = 4
LANES = 128
MESH = pl.DeviceIdType.MESH
VMEM_LIMIT = 62_000_000
GROUPS = 2
CHUNKS = 8
EARLY = ()
PARTS = 7
BLOCKS = 4
LEAD = 0.5
SLACK = 0.3
DOWN = 2
PER = CHUNKS // GROUPS
STEPS = LINE * GROUPS
PIECES = CHUNKS + len(EARLY)
AHEAD = sorted({c * BLOCKS // CHUNKS for c in (0, *EARLY)})
ORDERS = ((3, 2, 1, 0), (3, 0, 2, 1), (0, 3, 1, 2), (0, 1, 2, 3))


def requantized(tokens):
    rows, width = tokens.shape
    blocks = tokens.astype(jnp.float32).reshape(rows, -1, 16)
    largest = jnp.max(jnp.abs(blocks), axis=2)
    scales = (jnp.maximum(largest, 0.25) / 9.0).astype(jnp.bfloat16).astype(jnp.float32)
    divided = blocks / scales[:, :, None]
    payload = jnp.clip(divided, -6.0, 6.0).astype(jnp.bfloat16).astype(jnp.float32)
    return (payload * scales[:, :, None]).astype(jnp.bfloat16).reshape(rows, width)


def quantize_at(ref):
    rows, width = ref.shape
    many = PARTS
    square = (LANES, LANES)
    source = lax.broadcasted_iota(jnp.int32, square, 0)
    target = lax.broadcasted_iota(jnp.int32, square, 1)
    spread = jnp.where(source == target // 16 * 16 + 15, 1.0, 0.0).astype(ref.dtype)

    def body(i, carry):
        tiles, tops = [], []
        for u in range(many):
            at = pl.ds(pl.multiple_of((i * many + u) * LANES, LANES), LANES)
            values = ref[:, at]
            tiles.append((at, values))
            top = jnp.abs(values)
            for distance in (1, 2, 4, 8):
                top = jnp.maximum(top, pltpu.roll(top, distance, 1))
            tops.append(top)
        largest = jnp.dot(
            jnp.concatenate(tops, axis=0), spread, preferred_element_type=jnp.float32
        )
        results = []
        for u in range(many):
            at, values = tiles[u]
            scales = jnp.maximum(largest[u * rows : (u + 1) * rows], 0.25) / 9.0
            scales = scales.astype(jnp.bfloat16).astype(jnp.float32)
            payload = jnp.clip(values.astype(jnp.float32) / scales, -6.0, 6.0)
            payload = payload.astype(jnp.bfloat16).astype(jnp.float32)
            results.append((payload * scales).astype(ref.dtype))
        for u in range(many):
            ref[:, tiles[u][0]] = results[u]
        return carry

    lax.fori_loop(0, width // LANES // many, body, 0)


def row_of(piece):
    return piece if piece < CHUNKS else EARLY[piece - CHUNKS]


def in_order():
    return sorted(range(PIECES), key=lambda piece: (row_of(piece) // PER, piece))


def down_line():
    ranks = {piece: rank for rank, piece in enumerate(in_order())}
    ready = {
        z: {(z, piece): max(0, piece - CHUNKS + 2) for piece in range(PIECES)}
        for z in range(LINE)
    }
    sends = {z: [] for z in range(LINE)}
    for slot in range(8 * PIECES):
        for z in range(LINE - 1, 0, -1):
            able = [key for key, when in ready[z].items() if when <= slot]
            if able:
                owner, piece = min(able, key=lambda key: (-key[0], ranks[key[1]]))
                del ready[z][owner, piece]
                sends[z].append((slot, owner, piece))
                if z - 1 > 0:
                    ready[z - 1][owner, piece] = slot + 1
    return sends


def flip(order):
    return tuple(LINE - 1 - owner for owner in order)


FIRST, START = -1, 0
BACK = 4 * 512 / 7168 / GROUPS * CHUNKS / LINE


def before(k):
    return 1 + 3 * k


def middle(k):
    return 2 + 3 * k


def after(k):
    return 3 + 3 * k


LAST = after(STEPS)


def crossings(g):
    return [c for c in range(g * PER, g * PER + PER) if c not in EARLY]


def due(k):
    each = [len(crossings(g)) + BACK for g in range(GROUPS)]
    return LEAD + len(EARLY) + CHUNKS + k // GROUPS * sum(each) + sum(each[: k % GROUPS + 1])


def ready_at(k):
    return due(k) + 2


def gap_of(time, least):
    k = least
    while k < STEPS - 1 and due(k + 1) - SLACK < time:
        k += 1
    return k


def climb(orders):
    down = down_line()
    took = CHUNKS / GROUPS / PARTS
    came = {z: {} for z in range(LINE)}
    adds = {z: [] for z in range(LINE)}
    for z in range(LINE - 1):
        free = max(slot for slot, o, piece in down[LINE - 1 - z]) + 1
        todo = []
        for k in range(STEPS):
            o, g = orders[z][k // GROUPS], k % GROUPS
            if o > z:
                for n in range(PARTS):
                    when = ready_at(k) + 0.1 * n
                    place = k
                    if z > 0:
                        place = gap_of(came[z][o, g, n], k)
                        when = max(came[z][o, g, n], ready_at(place))
                    todo.append((place, when, o, g, n))
        for place, when, o, g, n in sorted(todo):
            free = max(free, when) + took
            came[z + 1][o, g, n] = free + 0.3
            adds[z].append((place, when, o, g, n))
    return came, adds


def script(z):
    last = LINE - 1
    down = down_line()
    up = {p: [(slot, last - o, c) for slot, o, c in down[last - p]] for p in range(LINE)}
    moves = [(slot, "down", o, c) for slot, o, c in down[z]]
    moves += [(slot, "up", o, c) for slot, o, c in up[z]]
    arrival = {(z, c): 0 for c in range(CHUNKS)}
    if z < last:
        arrival.update({(o, c): slot + 1 for slot, o, c in down[z + 1]})
    if z > 0:
        arrival.update({(o, c): slot + 1 for slot, o, c in up[z - 1]})
    steps = [(ORDERS[z][k // GROUPS], k % GROUPS) for k in range(STEPS)]
    chunks = [[(o, c) for c in crossings(g)] for o, g in steps]
    raw = []

    def add(place, rank, op):
        raw.append((place, rank, len(raw), op))

    for i, c in enumerate(EARLY):
        add(FIRST, 0.5, ("cross", z, c))
    for slot, way, o, piece in moves:
        if slot == 0:
            add(FIRST, 0, ("line", way, o, piece))
        elif slot <= due(0) - SLACK:
            add(START, slot, ("line", way, o, piece))
        else:
            add(after(min(STEPS - 2, gap_of(slot, 0))), slot, ("line", way, o, piece))
    for i in range(BLOCKS):
        if i not in AHEAD:
            add(START, i * CHUNKS / BLOCKS - 0.8, ("quantize", i))
    slow = CHUNKS / DOWN
    for i in range(DOWN):
        add(FIRST, 1, ("weights", i))
        add(START, len(EARLY) + (i + 1) * slow + 0.6, ("weights y", i))
        when = len(EARLY) + (i + 2) * slow + 1.1
        add(START if when < due(0) else before(0), when, ("weights x", i))
    latest = 0
    for o, c in chunks[0] + chunks[1][:1]:
        latest = max(latest, arrival[o, c] + 0.2)
        add(START, latest, ("cross", o, c))
    for k in range(STEPS):
        o, g = steps[k]
        for c in range(g * PER, g * PER + PER):
            add(before(k), 0, ("arrived", o, c))
            if c in EARLY and o != z:
                add(before(k), 0.5, ("arrived", o, CHUNKS + EARLY.index(c)))
            else:
                add(before(k), 1, ("crossed", o, c))
            add(middle(k), 2, ("free", o, c))
        if k + 1 < STEPS:
            for o, c in chunks[k + 1][1:]:
                add(middle(k), 0, ("cross", o, c))
        if k + 2 < STEPS:
            add(after(k), -1, ("cross",) + chunks[k + 2][0])
    flipped = [flip(ORDERS[last - p]) for p in range(LINE)]
    came_up, adds_up = climb(ORDERS)
    came_down, adds_down = climb(flipped)
    came, adds = {}, []
    if z > 0:
        for key, when in came_up[z].items():
            came[key] = max(came.get(key, 0), when)
        if z < last:
            adds += adds_up[z]
    if z < last:
        for (o, g, n), when in came_down[last - z].items():
            came[last - o, g, n] = max(came.get((last - o, g, n), 0), when)
        if z > 0:
            adds += [(k, when, last - o, g, n) for k, when, o, g, n in adds_down[last - z]]
    for k, when, o, g, n in sorted(adds):
        add(after(k), when, ("add", o, g, n))
    for g in range(GROUPS):
        own = [k for k in range(STEPS) if steps[k] == (z, g)][0]
        for n in range(PARTS):
            k = gap_of(came[z, g, n], own)
            add(after(k), max(came[z, g, n], ready_at(k)), ("finish", z, g, n))
    waited, sent, freed = set(), [], set()
    done = collections.defaultdict(list)
    for place, rank, number, op in sorted(raw):
        out = done[place]
        kind, key = op[0], op[-2:]
        if kind in ("add", "finish"):
            if out and out[-1][:3] == op[:3] and out[-1][4] == op[3]:
                out[-1] = out[-1][:4] + (op[3] + 1,)
            else:
                out.append(op + (op[3] + 1,))
            continue
        if kind in ("line", "cross", "arrived") and key not in waited:
            if key[0] != z:
                waited.add(key)
                out.append(("wait",) + key)
            elif key[1] >= CHUNKS:
                waited.add(key)
                out.append(("crossed", z, EARLY[key[1] - CHUNKS]))
        if kind == "crossed":
            early = EARLY.index(key[1]) + CHUNKS if key[1] in EARLY else None
            if early is not None and key[0] == z:
                if (z, early) not in waited:
                    waited.add((z, early))
                    out.append(op)
                continue
        if kind == "arrived":
            continue
        if kind in ("line", "cross"):
            assert key not in freed
            sent.append((op[1] if kind == "line" else "cross",) + key)
        if kind == "free":
            freed.add(key)
            for item in list(sent):
                if item[1:] == key:
                    sent.remove(item)
                    out.append(("sent",) + item)
            continue
        out.append(op)
    assert len(freed) == LINE * CHUNKS
    for item in sent:
        done[LAST].append(("sent",) + item)
    return done


def layer(
    tokens_ref,
    ids_ref,
    affinity_ref,
    gate_ref,
    up_ref,
    down_ref,
    out_ref,
    x_ref,
    wg_ref,
    wu_ref,
    wd_ref,
    hid_ref,
    peer_ref,
    got_ref,
    shares_ref,
    local,
    line_send,
    line_recv,
    cross_send,
    cross_recv,
    hid_send,
    hid_recv,
    part_send,
    part_recv,
    share_send,
    share_recv,
    w_send,
    w_recv,
):
    me, dp = lax.axis_index("ep"), lax.axis_index("dp")
    here, y = me // 2, lax.rem(me, 2)
    other = 1 - y
    last = LINE - 1
    peer = {"ep": 2 * here + other}
    twin = {"dp": dp + 1 - 2 * lax.rem(dp, 2)}
    across = {"dp": lax.rem(dp + 2, 4)}
    rows, width = out_ref.shape
    lot = rows // GROUPS
    size = rows // CHUNKS
    part = width // PARTS
    inner = wg_ref.shape[1]
    scripts = [script(z) for z in range(LINE)]

    def chunk(o, c):
        g, i = c // PER, c % PER
        return x_ref.at[o, g, pl.ds(pl.multiple_of(y * lot + i * size, size), size), :]

    def crossing(o, c):
        g, i = c // PER, c % PER
        return x_ref.at[o, g, pl.ds(pl.multiple_of(other * lot + i * size, size), size), :]

    def remote(source, place, send, recv, target):
        return pltpu.make_async_remote_copy(
            src_ref=source,
            dst_ref=place,
            send_sem=send,
            recv_sem=recv,
            device_id=target,
            device_id_type=MESH,
        )

    def line(way, o, c):
        target = {"ep": me + 2 if way == "up" else me - 2}
        place = chunk(o, c) if c < CHUNKS else crossing(o, EARLY[c - CHUNKS])
        return remote(
            place, place, line_send.at[0 if way == "up" else 1, o, c], line_recv.at[o, c], target
        )

    def cross(o, c):
        place = chunk(o, c)
        return remote(place, place, cross_send.at[o, c], cross_recv.at[o, c], peer)

    quarter = down_ref.shape[1] // 4
    piece = quarter // DOWN

    def rows_of(q, i):
        return pl.ds(pl.multiple_of(q * quarter + i * piece, piece), piece)

    def weight(kind, half, q, i, target):
        place = wd_ref.at[half, rows_of(q, i), :]
        source = down_ref.at[0, rows_of(q, i), :] if kind == 0 else place
        return remote(source, place, w_send.at[kind, i], w_recv.at[kind, i], target)

    q_mine, q_across = dp, lax.rem(dp + 2, 4)
    twin_dp = dp + 1 - 2 * lax.rem(dp, 2)
    q_twin, q_twin_across = twin_dp, lax.rem(twin_dp + 2, 4)

    def partial(z, o, g, n, way):
        step = 1 if way == "up" else -1
        nearest = isinstance(z, int) and z + step == o
        slot = LINE if way == "down" and nearest else o
        return part_copy(o, slot, g, n, {"ep": me + 2 * step})

    def part_copy(o, slot, g, n, target):
        columns = pl.ds(pl.multiple_of(n * part, part), part)
        source = x_ref.at[o, g, pl.ds(pl.multiple_of(y * lot, lot), lot), columns]
        return remote(
            source,
            got_ref.at[slot, g, :, columns],
            part_send.at[o, g, n],
            part_recv.at[slot, g, n],
            target,
        )

    def got_wait(slot, g, n):
        columns = pl.ds(pl.multiple_of(n * part, part), part)
        place = got_ref.at[slot, g, :, columns]
        remote(place, place, part_send.at[0, g, n], part_recv.at[slot, g, n], peer).wait_recv()

    def sum_into(target, at, sources):
        step = 16

        def body(i, carry):
            lines = pl.ds(pl.multiple_of(i * step, step), step)
            total = sources[0][lines, at].astype(jnp.float32)
            for source in sources[1:]:
                total = total + source[lines, at].astype(jnp.float32)
            target[lines, at] = total.astype(target.dtype)
            return carry

        lax.fori_loop(0, lot // step, body, 0)

    def quantize(i):
        block = rows // BLOCKS
        g, at = i * block // lot, i * block % lot
        lines = pl.ds(pl.multiple_of(y * lot + at, block), block)
        quantize_at(x_ref.at[here, g, lines, :])

    def run(z, op):
        kind = op[0]
        if kind == "wait":
            line("up", *op[1:]).wait_recv()
        elif kind == "line":
            line(*op[1:]).start()
        elif kind == "cross":
            cross(*op[1:]).start()
        elif kind == "crossed":
            place = crossing(*op[1:])
            o, c = op[1:]
            remote(place, place, cross_send.at[o, c], cross_recv.at[o, c], peer).wait_recv()
        elif kind == "sent":
            way, o, c = op[1:]
            (cross(o, c) if way == "cross" else line(way, o, c)).wait_send()
        elif kind == "quantize":
            quantize(op[1])
        elif kind == "weights":
            weight(0, y, q_mine, op[1], peer).start()
        elif kind == "weights y":
            weight(0, other, q_mine, op[1], peer).wait_recv()
            weight(1, other, q_mine, op[1], across).start()
            weight(2, other, q_mine, op[1], twin).start()
        elif kind == "weights x":
            weight(1, other, q_across, op[1], across).wait_recv()
            weight(3, other, q_across, op[1], twin).start()
        elif kind == "add":
            o, g, begin, end = op[1:]
            mine = x_ref.at[o, g, pl.ds(pl.multiple_of(y * lot, lot), lot), :]

            def body(n, carry):
                got_wait(o, g, n)
                at = pl.ds(pl.multiple_of(n * part, part), part)
                sum_into(mine, at, [mine, got_ref.at[o, g]])
                partial(z, o, g, n, "up" if o > z else "down").start()
                return carry

            lax.fori_loop(begin, end, body, 0)
        elif kind == "finish":
            g, begin, end = op[2:]
            mine = x_ref.at[z, g, pl.ds(pl.multiple_of(y * lot, lot), lot), :]
            slots = ([z] if z > 0 else []) + ([LINE] if z < last else [])

            def body(n, carry):
                for slot in slots:
                    got_wait(slot, g, n)
                at = pl.ds(pl.multiple_of(n * part, part), part)
                sum_into(
                    out_ref.at[pl.ds(g * lot, lot), :],
                    at,
                    [mine] + [got_ref.at[slot, g] for slot in slots],
                )
                return carry

            lax.fori_loop(begin, end, body, 0)
        else:
            raise ValueError(kind)

    def play(place):
        for z in range(LINE):
            ops = scripts[z][place]
            if ops:

                @pl.when(here == z)
                def _(z=z, ops=ops):
                    for op in ops:
                        run(z, op)

    def play_in(kind, k):
        for z in range(LINE):

            @pl.when(here == z)
            def _(z=z):
                for step in range(STEPS):
                    ops = scripts[z][kind(step)]
                    if ops:

                        @pl.when(k == step)
                        def _(ops=ops):
                            for op in ops:
                                run(z, op)

    own_rows = pl.ds(pl.multiple_of(y * lot, lot), lot)
    loads = []

    def load(source, place):
        copy = pltpu.make_async_copy(source, place, local.at[len(loads)])
        loads.append(copy)
        copy.start()

    for g in range(GROUPS):
        load(tokens_ref.at[pl.ds(g * lot, lot), :], x_ref.at[here, g, own_rows, :])
    load(gate_ref.at[0], wg_ref)
    load(up_ref.at[0], wu_ref)
    load(down_ref.at[0], wd_ref.at[y])
    barrier = pltpu.get_barrier_semaphore()
    targets = [{"ep": lax.rem(me + 2 * step, 2 * LINE)} for step in range(1, LINE)]
    targets += [peer, twin, across]
    for target in targets:
        pl.semaphore_signal(barrier, inc=1, device_id=target, device_id_type=MESH)

    for copy in loads[:GROUPS]:
        copy.wait()
    choices = ids_ref.shape[0]
    names = lax.broadcasted_iota(jnp.int32, shares_ref.shape[1:], 0)
    whole = sum(affinity_ref[i : i + 1, :] for i in range(choices))
    shares_ref[here] = sum(
        jnp.where(ids_ref[i : i + 1, :] == names, affinity_ref[i : i + 1, :] / whole, 0.0)
        for i in range(choices)
    )
    for i in AHEAD:
        quantize(i)
    pl.semaphore_wait(barrier, len(targets))
    play(FIRST)
    shares = []
    for step in range(1, LINE):
        target = {"ep": lax.rem(me + 2 * step, 2 * LINE)}
        mine = shares_ref.at[here]
        copy = remote(mine, mine, share_send.at[step], share_recv.at[step], target)
        copy.start()
        shares.append(copy)
    play(START)
    for copy in loads[GROUPS:]:
        copy.wait()
    for copy in shares:
        copy.wait()

    def order(k):
        b = k // GROUPS
        value = jnp.int32(0)
        for z in range(LINE):
            for i in range(LINE):
                value = jnp.where((here == z) & (b == i), ORDERS[z][i], value)
        return value

    half = inner // 2

    def step_of(k, carry):
        o, g = order(k), lax.rem(k, GROUPS)
        play_in(before, k)

        def hidden(j, c):
            at = pl.ds(pl.multiple_of(j * half, half), half)
            x = x_ref[o, g]
            gate = jnp.dot(x, wg_ref[:, at], preferred_element_type=jnp.float32)
            upward = jnp.dot(x, wu_ref[:, at], preferred_element_type=jnp.float32)
            hid_ref[o, g, :, at] = (jax.nn.silu(gate) * upward).astype(hid_ref.dtype)
            return c

        lax.fori_loop(0, 2, hidden, 0)
        other_rows = pl.ds(pl.multiple_of(other * lot, lot), lot)
        back = remote(
            hid_ref.at[o, g, other_rows, :],
            peer_ref.at[o, g],
            hid_send.at[o, g],
            hid_recv.at[o, g],
            peer,
        )
        back.start()
        play_in(middle, k)

        @pl.when(k == 0)
        def _():
            for i in range(DOWN):
                weight(2, other, q_twin, i, twin).wait_recv()
                weight(3, other, q_twin_across, i, twin).wait_recv()

        back.wait()
        row = shares_ref[o, pl.ds(here, 1), :]
        square = (lot, row.shape[1])
        lane = lax.broadcasted_iota(jnp.int32, square, 1)
        line_of = lax.broadcasted_iota(jnp.int32, square, 0)
        share = jnp.sum(
            jnp.where(lane == line_of + g * lot, jnp.broadcast_to(row, square), 0.0),
            axis=1,
            keepdims=True,
        )
        begins = ((here == 0) & (o != 0)) | ((here == last) & (o != last))
        slot = jnp.where((here == last) & (o == last - 1), LINE, o)
        onward = jnp.where(here == 0, me + 2, me - 2)

        def down(n, c):
            at = pl.ds(pl.multiple_of(n * part, part), part)
            total = jnp.dot(
                hid_ref[o, g, own_rows, :], wd_ref[y, :, at], preferred_element_type=jnp.float32
            ) + jnp.dot(peer_ref[o, g], wd_ref[other, :, at], preferred_element_type=jnp.float32)
            x_ref[o, g, own_rows, at] = (total * share).astype(x_ref.dtype)

            @pl.when(begins)
            def _():
                part_copy(o, slot, g, n, {"ep": onward}).start()

            return c

        lax.fori_loop(0, PARTS, down, 0)
        play_in(after, k)
        return carry

    lax.fori_loop(0, STEPS, step_of, 0)

    def drain(i, carry):
        o, g = i // GROUPS, lax.rem(i, GROUPS)

        @pl.when(o != here)
        def _():
            def body(n, c):
                part_copy(o, o, g, n, peer).wait_send()
                return c

            lax.fori_loop(0, PARTS, body, 0)

        return carry

    lax.fori_loop(0, STEPS, drain, 0)
    play(LAST)
    for i in range(DOWN):
        weight(0, y, q_mine, i, peer).wait_send()
        weight(1, other, q_mine, i, across).wait_send()
        weight(2, other, q_mine, i, twin).wait_send()
        weight(3, other, q_across, i, twin).wait_send()


def fused(tokens, expert_ids, affinity, w_gate, w_up, w_down):
    rows, width = tokens.shape
    inner = w_gate.shape[2]
    lot = rows // GROUPS
    kind = tokens.dtype
    dma = pltpu.SemaphoreType.DMA
    anywhere = pl.BlockSpec(memory_space=pl.ANY)
    inside = pl.BlockSpec(memory_space=pltpu.VMEM)
    return pl.pallas_call(
        layer,
        out_shape=jax.ShapeDtypeStruct((rows, width), kind),
        in_specs=[anywhere, inside, inside, anywhere, anywhere, anywhere],
        out_specs=inside,
        scratch_shapes=[
            pltpu.VMEM((LINE, GROUPS, 2 * lot, width), kind),
            pltpu.VMEM((width, inner), kind),
            pltpu.VMEM((width, inner), kind),
            pltpu.VMEM((2, inner, width), kind),
            pltpu.VMEM((LINE, GROUPS, 2 * lot, inner), kind),
            pltpu.VMEM((LINE, GROUPS, lot, inner), kind),
            pltpu.VMEM((LINE + 1, GROUPS, lot, width), kind),
            pltpu.VMEM((LINE, 8, rows), affinity.dtype),
            dma((GROUPS + 3,)),
            dma((2, LINE, PIECES)),
            dma((LINE, PIECES)),
            dma((LINE, CHUNKS)),
            dma((LINE, CHUNKS)),
            dma((LINE, GROUPS)),
            dma((LINE, GROUPS)),
            dma((LINE, GROUPS, PARTS)),
            dma((LINE + 1, GROUPS, PARTS)),
            dma((LINE,)),
            dma((LINE,)),
            dma((4, DOWN)),
            dma((4, DOWN)),
        ],
        compiler_params=pltpu.CompilerParams(
            collective_id=0, has_side_effects=True, vmem_limit_bytes=VMEM_LIMIT
        ),
        name="layer",
    )(tokens, expert_ids.T, affinity.T, w_gate, w_up, w_down)


def on_device(tokens, expert_ids, affinity, w_gate, w_up, w_down):
    n = lax.axis_size("ep")
    experts = n // 2
    own = lax.axis_index("ep") // 2
    rows, width = tokens.shape
    by_line = (
        experts == LINE
        and lax.axis_size("dp") == 4
        and rows == LANES
        and width % (PARTS * LANES) == 0
    )
    if by_line:
        return fused(tokens, expert_ids, affinity, w_gate, w_up, w_down)
    weights = affinity / jnp.sum(affinity, axis=1, keepdims=True)
    padded = -(-experts // 8) * 8
    names = jnp.arange(padded, dtype=jnp.int32)[:, None]
    shares = sum(
        jnp.where(expert_ids[:, k][None, :] == names, weights[:, k][None, :], 0.0)
        for k in range(weights.shape[1])
    )
    every = lax.all_gather(requantized(tokens), "ep", axis=0, tiled=False)
    shares = lax.all_gather(shares, "ep", axis=0, tiled=False)
    every = every.reshape(n * rows, width)
    share = lax.dynamic_slice_in_dim(shares, own, 1, axis=1).reshape(n * rows, 1)
    gate = jnp.dot(every, w_gate[0], preferred_element_type=jnp.float32)
    upward = jnp.dot(every, w_up[0], preferred_element_type=jnp.float32)
    hidden = (jax.nn.silu(gate) * upward).astype(jnp.bfloat16)
    partial = jnp.dot(hidden, w_down[0], preferred_element_type=jnp.float32)
    scaled = (partial * share).astype(jnp.bfloat16)
    return lax.psum_scatter(scaled, "ep", scatter_dimension=0, tiled=True)


def solution(mesh):
    in_specs = (
        P(("dp", "ep"), None),
        P(("dp", "ep"), None),
        P(("dp", "ep"), None),
        P("ep", None, None),
        P("ep", None, None),
        P("ep", None, None),
    )
    return jax.shard_map(
        on_device, mesh=mesh, in_specs=in_specs, out_specs=P(("dp", "ep"), None), check_vma=False
    )
```

```python
import collections
import functools

import jax
import jax.numpy as jnp
from jax import lax
from jax.experimental import pallas as pl
from jax.experimental.pallas import tpu as pltpu
from jax.sharding import PartitionSpec as P

LINE = 4
LANES = 128
MESH = pl.DeviceIdType.MESH
VMEM_LIMIT = 62_000_000
GROUPS = 2
CHUNKS = 8
EARLY = (1, 5)
PARTS = 7
BLOCKS = 4
LEAD = 0.5
SLACK = 0.3
FAR = 2
HOP = 2
LATE = 1.4
DOWN = 4
PER = CHUNKS // GROUPS
STEPS = LINE * GROUPS
PIECES = CHUNKS + len(EARLY)
AHEAD = (0,)
END = ((3, 0), (3, 1), (2, 0), (2, 1), (1, 0), (0, 0), (1, 1), (0, 1))
INNER = ((3, 0), (3, 1), (0, 0), (0, 1), (2, 0), (2, 1), (1, 0), (1, 1))


def requantized(tokens):
    rows, width = tokens.shape
    blocks = tokens.astype(jnp.float32).reshape(rows, -1, 16)
    largest = jnp.max(jnp.abs(blocks), axis=2)
    scales = (jnp.maximum(largest, 0.25) / 9.0).astype(jnp.bfloat16).astype(jnp.float32)
    divided = blocks / scales[:, :, None]
    payload = jnp.clip(divided, -6.0, 6.0).astype(jnp.bfloat16).astype(jnp.float32)
    return (payload * scales[:, :, None]).astype(jnp.bfloat16).reshape(rows, width)


def quantize_at(ref):
    rows, width = ref.shape
    many = PARTS
    square = (LANES, LANES)
    source = lax.broadcasted_iota(jnp.int32, square, 0)
    target = lax.broadcasted_iota(jnp.int32, square, 1)
    spread = jnp.where(source == target // 16 * 16 + 15, 1.0, 0.0).astype(ref.dtype)

    def body(i, carry):
        tiles, tops = [], []
        for u in range(many):
            at = pl.ds(pl.multiple_of((i * many + u) * LANES, LANES), LANES)
            values = ref[:, at]
            tiles.append((at, values))
            top = jnp.abs(values)
            for distance in (1, 2, 4, 8):
                top = jnp.maximum(top, pltpu.roll(top, distance, 1))
            tops.append(top)
        largest = jnp.dot(
            jnp.concatenate(tops, axis=0), spread, preferred_element_type=jnp.float32
        )
        results = []
        for u in range(many):
            at, values = tiles[u]
            scales = jnp.maximum(largest[u * rows : (u + 1) * rows], 0.25) / 9.0
            scales = scales.astype(jnp.bfloat16).astype(jnp.float32)
            payload = jnp.clip(values.astype(jnp.float32) / scales, -6.0, 6.0)
            payload = payload.astype(jnp.bfloat16).astype(jnp.float32)
            results.append((payload * scales).astype(ref.dtype))
        for u in range(many):
            ref[:, tiles[u][0]] = results[u]
        return carry

    lax.fori_loop(0, width // LANES // many, body, 0)


def row_of(piece):
    return piece if piece < CHUNKS else EARLY[piece - CHUNKS]


def early_at(z):
    return EARLY if 0 < z < LINE - 1 else EARLY[:FAR]


def in_order():
    return sorted(range(PIECES), key=lambda piece: (row_of(piece) // PER, piece))


def down_line():
    ranks = {piece: rank for rank, piece in enumerate(in_order())}
    ready = {
        z: {(z, piece): max(0, 2 * (piece - CHUNKS) + 2) for piece in range(PIECES)}
        for z in range(LINE)
    }
    sends = {z: [] for z in range(LINE)}
    for slot in range(8 * PIECES):
        for z in range(LINE - 1, 0, -1):
            able = [
                key
                for key, when in ready[z].items()
                if when <= slot and (key[1] < CHUNKS or row_of(key[1]) in early_at(z - 1))
            ]
            if able:
                owner, piece = min(able, key=lambda key: (-key[0], ranks[key[1]]))
                del ready[z][owner, piece]
                sends[z].append((slot, owner, piece))
                if z - 1 > 0:
                    ready[z - 1][owner, piece] = slot + HOP
    return sends


def turn(block):
    early = sorted({c * BLOCKS // CHUNKS for c in EARLY} - set(AHEAD))
    if block in early:
        return 0.1 + early.index(block)
    return block * CHUNKS / BLOCKS - 0.8


def settled(c):
    block = c * BLOCKS // CHUNKS
    return 0 if block in AHEAD else turn(block) + 0.05


def starts(z, moves, arrival):
    latest, found = 0, []
    for number, (slot, owner, piece) in enumerate(moves):
        able = arrival.get((owner, piece), 0)
        if owner == z:
            tail = all(key[1] == z for key in moves[number:])
            able = latest if tail and z in (1, LINE - 2) else max(0, slot - 1)
            able = max(able, settled(row_of(piece)))
            if piece >= CHUNKS:
                able = max(able, 2 * (piece - CHUNKS) + 1.5)
        latest = max(latest, able)
        found.append((latest, owner, piece))
    return found


def flip(order):
    return tuple((LINE - 1 - owner, g) for owner, g in order)


ORDERS = (END, INNER, flip(INNER), flip(END))


FIRST, START = -1, 0
BACK = 4 * 512 / 7168 / GROUPS * CHUNKS / LINE


def before(k):
    return 1 + 3 * k


def middle(k):
    return 2 + 3 * k


def after(k):
    return 3 + 3 * k


LAST = after(STEPS)


def crossings(g, early):
    return [c for c in range(g * PER, g * PER + PER) if c not in early]


def due(k, z):
    total = LEAD + CHUNKS + len(EARLY)
    for o, g in ORDERS[z][: k + 1]:
        total += len(crossings(g, EARLY if o == z else early_at(z))) + BACK
    return total


def ready_at(k, z):
    return due(k, z) + 2


def gap_of(time, least, z):
    k = least
    while k < STEPS - 1 and due(k + 1, z) - SLACK < time:
        k += 1
    return k


def climb(orders):
    down = down_line()
    took = CHUNKS / GROUPS / PARTS
    came = {z: {} for z in range(LINE)}
    adds = {z: [] for z in range(LINE)}
    for z in range(LINE - 1):
        free = max(slot for slot, o, piece in down[LINE - 1 - z]) + 1
        todo = []
        for k in range(STEPS):
            o, g = orders[z][k]
            if o > z:
                for n in range(PARTS):
                    when = ready_at(k, z) + 0.1 * n
                    place = k
                    if z > 0:
                        place = gap_of(came[z][o, g, n], k, z)
                        when = max(came[z][o, g, n], ready_at(place, z))
                    todo.append((place, when, o, g, n))
        for place, when, o, g, n in sorted(todo):
            free = max(free, when) + took
            came[z + 1][o, g, n] = free + 0.3
            adds[z].append((place, when, o, g, n))
    return came, adds


def script(z):
    last = LINE - 1
    down = down_line()
    up = {p: [(slot, last - o, c) for slot, o, c in down[last - p]] for p in range(LINE)}
    arrival = {(z, c): settled(c) for c in range(CHUNKS)}
    if z < last:
        arrival.update({(o, c): slot + LATE for slot, o, c in down[z + 1]})
    if z > 0:
        arrival.update({(o, c): slot + LATE for slot, o, c in up[z - 1]})
    moves = [(slot, "down", o, c) for slot, o, c in starts(z, down[z], arrival)]
    moves += [(slot, "up", o, c) for slot, o, c in starts(z, up[z], arrival)]
    steps = ORDERS[z]
    chunks = [
        [(o, c) for c in crossings(g, EARLY if o == z else early_at(z))] for o, g in steps
    ]
    raw = []

    def add(place, rank, op):
        raw.append((place, rank, len(raw), op))

    begun = {}
    for c in EARLY:
        block = c * BLOCKS // CHUNKS
        begun[c] = 0.5 if block in AHEAD else turn(block) + 0.9
        add(FIRST if block in AHEAD else START, begun[c], ("cross", z, c))
    for slot, way, o, piece in moves:
        if slot == 0 and row_of(piece) * BLOCKS // CHUNKS in AHEAD:
            add(FIRST, 0, ("line", way, o, piece))
        elif slot <= due(0, z) - SLACK:
            add(START, slot, ("line", way, o, piece))
        else:
            k = min(STEPS - 2, gap_of(slot, 0, z))
            place = middle(k) if slot <= due(k, z) + 0.6 else after(k)
            add(place, 1 + slot / 100, ("line", way, o, piece))
    for i in range(BLOCKS):
        if i not in AHEAD:
            add(START, turn(i), ("quantize", i))
    slow = CHUNKS / DOWN
    for i in range(DOWN):
        add(FIRST if i == 0 else START, max(1, max(begun.values()) + 0.01), ("weights", i))
        add(START, len(EARLY) + (i + 1) * slow + 0.6, ("weights y", i))
        when = len(EARLY) + (i + 2) * slow + 1.1
        add(START if when < due(0, z) else before(0), when, ("weights x", i))
    latest = 0
    for o, c in chunks[0] + chunks[1][:1]:
        latest = max(latest, arrival[o, c] + 0.2)
        add(START, latest, ("cross", o, c))
    for k in range(STEPS):
        o, g = steps[k]
        for c in range(g * PER, g * PER + PER):
            add(before(k), 0, ("arrived", o, c))
            if o != z and c in early_at(z):
                add(before(k), 0.5, ("arrived", o, CHUNKS + EARLY.index(c)))
            else:
                add(before(k), 1, ("crossed", o, c))
            add(middle(k), 2, ("free", o, c))
        if k + 1 < STEPS:
            for o, c in chunks[k + 1][1:]:
                add(middle(k), 0, ("cross", o, c))
        if k + 2 < STEPS:
            add(after(k), -1, ("cross",) + chunks[k + 2][0])
    flipped = [flip(ORDERS[last - p]) for p in range(LINE)]
    came_up, adds_up = climb(ORDERS)
    came_down, adds_down = climb(flipped)
    came, adds = {}, []
    if z > 0:
        for key, when in came_up[z].items():
            came[key] = max(came.get(key, 0), when)
        if z < last:
            adds += adds_up[z]
    if z < last:
        for (o, g, n), when in came_down[last - z].items():
            came[last - o, g, n] = max(came.get((last - o, g, n), 0), when)
        if z > 0:
            adds += [(k, when, last - o, g, n) for k, when, o, g, n in adds_down[last - z]]
    for k, when, o, g, n in sorted(adds):
        add(after(k), when, ("add", o, g, n))
    for g in range(GROUPS):
        own = [k for k in range(STEPS) if steps[k] == (z, g)][0]
        for n in range(PARTS):
            k = gap_of(came[z, g, n], own, z)
            add(after(k), max(came[z, g, n], ready_at(k, z)), ("finish", z, g, n))
    waited, sent, freed = set(), [], set()
    done = collections.defaultdict(list)
    for place, rank, number, op in sorted(raw):
        out = done[place]
        kind, key = op[0], op[-2:]
        if kind in ("add", "finish"):
            if out and out[-1][:3] == op[:3] and out[-1][4] == op[3]:
                out[-1] = out[-1][:4] + (op[3] + 1,)
            else:
                out.append(op + (op[3] + 1,))
            continue
        if kind in ("line", "cross", "arrived") and key not in waited:
            if key[0] != z:
                waited.add(key)
                out.append(("wait",) + key)
            elif key[1] >= CHUNKS:
                waited.add(key)
                out.append(("crossed", z, EARLY[key[1] - CHUNKS]))
        if kind == "crossed":
            early = EARLY.index(key[1]) + CHUNKS if key[1] in EARLY else None
            if early is not None and key[0] == z:
                if (z, early) not in waited:
                    waited.add((z, early))
                    out.append(op)
                continue
        if kind == "arrived":
            continue
        if kind in ("line", "cross"):
            assert key not in freed
            sent.append((op[1] if kind == "line" else "cross",) + key)
        if kind == "free":
            freed.add(key)
            for item in list(sent):
                if item[1:] == key:
                    sent.remove(item)
                    out.append(("sent",) + item)
            continue
        out.append(op)
    assert len(freed) == LINE * CHUNKS
    for item in sent:
        done[LAST].append(("sent",) + item)
    return done


def layer(
    tokens_ref,
    ids_ref,
    affinity_ref,
    gate_ref,
    up_ref,
    down_ref,
    out_ref,
    x_ref,
    wg_ref,
    wu_ref,
    wd_ref,
    hid_ref,
    peer_ref,
    got_ref,
    shares_ref,
    local,
    line_send,
    line_recv,
    cross_send,
    cross_recv,
    hid_send,
    hid_recv,
    part_send,
    part_recv,
    share_send,
    share_recv,
    w_send,
    w_recv,
):
    me, dp = lax.axis_index("ep"), lax.axis_index("dp")
    here, y = me // 2, lax.rem(me, 2)
    other = 1 - y
    last = LINE - 1
    peer = {"ep": 2 * here + other}
    twin = {"dp": dp + 1 - 2 * lax.rem(dp, 2)}
    across = {"dp": lax.rem(dp + 2, 4)}
    rows, width = out_ref.shape
    lot = rows // GROUPS
    size = rows // CHUNKS
    part = width // PARTS
    inner = wg_ref.shape[1]
    scripts = [script(z) for z in range(LINE)]

    def chunk(o, c):
        g, i = c // PER, c % PER
        return x_ref.at[o, g, pl.ds(pl.multiple_of(y * lot + i * size, size), size), :]

    def crossing(o, c):
        g, i = c // PER, c % PER
        return x_ref.at[o, g, pl.ds(pl.multiple_of(other * lot + i * size, size), size), :]

    def remote(source, place, send, recv, target):
        return pltpu.make_async_remote_copy(
            src_ref=source,
            dst_ref=place,
            send_sem=send,
            recv_sem=recv,
            device_id=target,
            device_id_type=MESH,
        )

    def line(way, o, c):
        target = {"ep": me + 2 if way == "up" else me - 2}
        place = chunk(o, c) if c < CHUNKS else crossing(o, EARLY[c - CHUNKS])
        return remote(
            place, place, line_send.at[0 if way == "up" else 1, o, c], line_recv.at[o, c], target
        )

    def cross(o, c):
        place = chunk(o, c)
        return remote(place, place, cross_send.at[o, c], cross_recv.at[o, c], peer)

    quarter = down_ref.shape[1] // 4
    piece = quarter // DOWN

    def rows_of(q, i):
        return pl.ds(pl.multiple_of(q * quarter + i * piece, piece), piece)

    def weight(kind, half, q, i, target):
        place = wd_ref.at[half, rows_of(q, i), :]
        source = down_ref.at[0, rows_of(q, i), :] if kind == 0 else place
        return remote(source, place, w_send.at[kind, i], w_recv.at[kind, i], target)

    q_mine, q_across = dp, lax.rem(dp + 2, 4)
    twin_dp = dp + 1 - 2 * lax.rem(dp, 2)
    q_twin, q_twin_across = twin_dp, lax.rem(twin_dp + 2, 4)

    def partial(z, o, g, n, way):
        step = 1 if way == "up" else -1
        nearest = isinstance(z, int) and z + step == o
        slot = LINE if way == "down" and nearest else o
        return part_copy(o, slot, g, n, {"ep": me + 2 * step})

    def part_copy(o, slot, g, n, target):
        columns = pl.ds(pl.multiple_of(n * part, part), part)
        source = x_ref.at[o, g, pl.ds(pl.multiple_of(y * lot, lot), lot), columns]
        return remote(
            source,
            got_ref.at[slot, g, :, columns],
            part_send.at[o, g, n],
            part_recv.at[slot, g, n],
            target,
        )

    def got_wait(slot, g, n):
        columns = pl.ds(pl.multiple_of(n * part, part), part)
        place = got_ref.at[slot, g, :, columns]
        remote(place, place, part_send.at[0, g, n], part_recv.at[slot, g, n], peer).wait_recv()

    def sum_into(target, at, sources):
        step = 16

        def body(i, carry):
            lines = pl.ds(pl.multiple_of(i * step, step), step)
            total = sources[0][lines, at].astype(jnp.float32)
            for source in sources[1:]:
                total = total + source[lines, at].astype(jnp.float32)
            target[lines, at] = total.astype(target.dtype)
            return carry

        lax.fori_loop(0, lot // step, body, 0)

    def quantize(i):
        block = rows // BLOCKS
        g, at = i * block // lot, i * block % lot
        lines = pl.ds(pl.multiple_of(y * lot + at, block), block)
        quantize_at(x_ref.at[here, g, lines, :])

    def run(z, op):
        kind = op[0]
        if kind == "wait":
            line("up", *op[1:]).wait_recv()
        elif kind == "line":
            line(*op[1:]).start()
        elif kind == "cross":
            cross(*op[1:]).start()
        elif kind == "crossed":
            place = crossing(*op[1:])
            o, c = op[1:]
            remote(place, place, cross_send.at[o, c], cross_recv.at[o, c], peer).wait_recv()
        elif kind == "sent":
            way, o, c = op[1:]
            (cross(o, c) if way == "cross" else line(way, o, c)).wait_send()
        elif kind == "quantize":
            quantize(op[1])
        elif kind == "weights":
            weight(0, y, q_mine, op[1], peer).start()
        elif kind == "weights y":
            weight(0, other, q_mine, op[1], peer).wait_recv()
            weight(1, other, q_mine, op[1], across).start()
            weight(2, other, q_mine, op[1], twin).start()
        elif kind == "weights x":
            weight(1, other, q_across, op[1], across).wait_recv()
            weight(3, other, q_across, op[1], twin).start()
        elif kind == "add":
            o, g, begin, end = op[1:]
            mine = x_ref.at[o, g, pl.ds(pl.multiple_of(y * lot, lot), lot), :]

            def body(n, carry):
                got_wait(o, g, n)
                at = pl.ds(pl.multiple_of(n * part, part), part)
                sum_into(mine, at, [mine, got_ref.at[o, g]])
                partial(z, o, g, n, "up" if o > z else "down").start()
                return carry

            lax.fori_loop(begin, end, body, 0)
        elif kind == "finish":
            g, begin, end = op[2:]
            mine = x_ref.at[z, g, pl.ds(pl.multiple_of(y * lot, lot), lot), :]
            slots = ([z] if z > 0 else []) + ([LINE] if z < last else [])

            def body(n, carry):
                for slot in slots:
                    got_wait(slot, g, n)
                at = pl.ds(pl.multiple_of(n * part, part), part)
                sum_into(
                    out_ref.at[pl.ds(g * lot, lot), :],
                    at,
                    [mine] + [got_ref.at[slot, g] for slot in slots],
                )
                return carry

            lax.fori_loop(begin, end, body, 0)
        else:
            raise ValueError(kind)

    def play(place):
        for z in range(LINE):
            ops = scripts[z][place]
            if ops:

                @pl.when(here == z)
                def _(z=z, ops=ops):
                    for op in ops:
                        run(z, op)

    def play_in(kind, k):
        for z in range(LINE):

            @pl.when(here == z)
            def _(z=z):
                for step in range(STEPS):
                    ops = scripts[z][kind(step)]
                    if ops:

                        @pl.when(k == step)
                        def _(ops=ops):
                            for op in ops:
                                run(z, op)

    own_rows = pl.ds(pl.multiple_of(y * lot, lot), lot)
    loads = []

    def load(source, place):
        copy = pltpu.make_async_copy(source, place, local.at[len(loads)])
        loads.append(copy)
        copy.start()

    for g in range(GROUPS):
        load(tokens_ref.at[pl.ds(g * lot, lot), :], x_ref.at[here, g, own_rows, :])
    load(gate_ref.at[0], wg_ref)
    load(up_ref.at[0], wu_ref)
    load(down_ref.at[0], wd_ref.at[y])
    barrier = pltpu.get_barrier_semaphore()
    targets = [{"ep": lax.rem(me + 2 * step, 2 * LINE)} for step in range(1, LINE)]
    targets += [peer, twin, across]
    for target in targets:
        pl.semaphore_signal(barrier, inc=1, device_id=target, device_id_type=MESH)

    for copy in loads[:GROUPS]:
        copy.wait()
    choices = ids_ref.shape[0]
    names = lax.broadcasted_iota(jnp.int32, shares_ref.shape[1:], 0)
    whole = sum(affinity_ref[i : i + 1, :] for i in range(choices))
    shares_ref[here] = sum(
        jnp.where(ids_ref[i : i + 1, :] == names, affinity_ref[i : i + 1, :] / whole, 0.0)
        for i in range(choices)
    )
    for i in AHEAD:
        quantize(i)
    pl.semaphore_wait(barrier, len(targets))
    play(FIRST)
    shares = []
    for step in range(1, LINE):
        target = {"ep": lax.rem(me + 2 * step, 2 * LINE)}
        mine = shares_ref.at[here]
        copy = remote(mine, mine, share_send.at[step], share_recv.at[step], target)
        copy.start()
        shares.append(copy)
    play(START)
    for copy in loads[GROUPS:]:
        copy.wait()
    for copy in shares:
        copy.wait()

    def order(k, which):
        value = jnp.int32(0)
        for z in range(LINE):
            for i in range(STEPS):
                if ORDERS[z][i][which]:
                    value = jnp.where((here == z) & (k == i), ORDERS[z][i][which], value)
        return value

    half = inner // 2

    def step_of(k, carry):
        o, g = order(k, 0), order(k, 1)
        play_in(before, k)

        def hidden(j, c):
            at = pl.ds(pl.multiple_of(j * half, half), half)
            x = x_ref[o, g]
            gate = jnp.dot(x, wg_ref[:, at], preferred_element_type=jnp.float32)
            upward = jnp.dot(x, wu_ref[:, at], preferred_element_type=jnp.float32)
            hid_ref[o, g, :, at] = (jax.nn.silu(gate) * upward).astype(hid_ref.dtype)
            return c

        lax.fori_loop(0, 2, hidden, 0)
        other_rows = pl.ds(pl.multiple_of(other * lot, lot), lot)
        back = remote(
            hid_ref.at[o, g, other_rows, :],
            peer_ref.at[o, g],
            hid_send.at[o, g],
            hid_recv.at[o, g],
            peer,
        )
        back.start()
        play_in(middle, k)

        @pl.when(k == 0)
        def _():
            for i in range(DOWN):
                weight(2, other, q_twin, i, twin).wait_recv()
                weight(3, other, q_twin_across, i, twin).wait_recv()

        back.wait()
        row = shares_ref[o, pl.ds(here, 1), :]
        square = (lot, row.shape[1])
        lane = lax.broadcasted_iota(jnp.int32, square, 1)
        line_of = lax.broadcasted_iota(jnp.int32, square, 0)
        share = jnp.sum(
            jnp.where(lane == line_of + g * lot, jnp.broadcast_to(row, square), 0.0),
            axis=1,
            keepdims=True,
        )
        begins = ((here == 0) & (o != 0)) | ((here == last) & (o != last))
        slot = jnp.where((here == last) & (o == last - 1), LINE, o)
        onward = jnp.where(here == 0, me + 2, me - 2)

        def down(n, c):
            at = pl.ds(pl.multiple_of(n * part, part), part)
            total = jnp.dot(
                hid_ref[o, g, own_rows, :], wd_ref[y, :, at], preferred_element_type=jnp.float32
            ) + jnp.dot(peer_ref[o, g], wd_ref[other, :, at], preferred_element_type=jnp.float32)
            x_ref[o, g, own_rows, at] = (total * share).astype(x_ref.dtype)

            @pl.when(begins)
            def _():
                part_copy(o, slot, g, n, {"ep": onward}).start()

            return c

        lax.fori_loop(0, PARTS, down, 0)
        play_in(after, k)
        return carry

    lax.fori_loop(0, STEPS, step_of, 0)

    def drain(i, carry):
        o, g = i // GROUPS, lax.rem(i, GROUPS)

        @pl.when(o != here)
        def _():
            def body(n, c):
                part_copy(o, o, g, n, peer).wait_send()
                return c

            lax.fori_loop(0, PARTS, body, 0)

        return carry

    lax.fori_loop(0, STEPS, drain, 0)
    play(LAST)
    for i in range(DOWN):
        weight(0, y, q_mine, i, peer).wait_send()
        weight(1, other, q_mine, i, across).wait_send()
        weight(2, other, q_mine, i, twin).wait_send()
        weight(3, other, q_across, i, twin).wait_send()


def fused(tokens, expert_ids, affinity, w_gate, w_up, w_down):
    rows, width = tokens.shape
    inner = w_gate.shape[2]
    lot = rows // GROUPS
    kind = tokens.dtype
    dma = pltpu.SemaphoreType.DMA
    anywhere = pl.BlockSpec(memory_space=pl.ANY)
    inside = pl.BlockSpec(memory_space=pltpu.VMEM)
    return pl.pallas_call(
        layer,
        out_shape=jax.ShapeDtypeStruct((rows, width), kind),
        in_specs=[anywhere, inside, inside, anywhere, anywhere, anywhere],
        out_specs=inside,
        scratch_shapes=[
            pltpu.VMEM((LINE, GROUPS, 2 * lot, width), kind),
            pltpu.VMEM((width, inner), kind),
            pltpu.VMEM((width, inner), kind),
            pltpu.VMEM((2, inner, width), kind),
            pltpu.VMEM((LINE, GROUPS, 2 * lot, inner), kind),
            pltpu.VMEM((LINE, GROUPS, lot, inner), kind),
            pltpu.VMEM((LINE + 1, GROUPS, lot, width), kind),
            pltpu.VMEM((LINE, 8, rows), affinity.dtype),
            dma((GROUPS + 3,)),
            dma((2, LINE, PIECES)),
            dma((LINE, PIECES)),
            dma((LINE, CHUNKS)),
            dma((LINE, CHUNKS)),
            dma((LINE, GROUPS)),
            dma((LINE, GROUPS)),
            dma((LINE, GROUPS, PARTS)),
            dma((LINE + 1, GROUPS, PARTS)),
            dma((LINE,)),
            dma((LINE,)),
            dma((4, DOWN)),
            dma((4, DOWN)),
        ],
        compiler_params=pltpu.CompilerParams(
            collective_id=0, has_side_effects=True, vmem_limit_bytes=VMEM_LIMIT
        ),
        name="layer",
    )(tokens, expert_ids.T, affinity.T, w_gate, w_up, w_down)


def on_device(tokens, expert_ids, affinity, w_gate, w_up, w_down):
    n = lax.axis_size("ep")
    experts = n // 2
    own = lax.axis_index("ep") // 2
    rows, width = tokens.shape
    by_line = (
        experts == LINE
        and lax.axis_size("dp") == 4
        and rows == LANES
        and width % (PARTS * LANES) == 0
    )
    if by_line:
        return fused(tokens, expert_ids, affinity, w_gate, w_up, w_down)
    weights = affinity / jnp.sum(affinity, axis=1, keepdims=True)
    padded = -(-experts // 8) * 8
    names = jnp.arange(padded, dtype=jnp.int32)[:, None]
    shares = sum(
        jnp.where(expert_ids[:, k][None, :] == names, weights[:, k][None, :], 0.0)
        for k in range(weights.shape[1])
    )
    every = lax.all_gather(requantized(tokens), "ep", axis=0, tiled=False)
    shares = lax.all_gather(shares, "ep", axis=0, tiled=False)
    every = every.reshape(n * rows, width)
    share = lax.dynamic_slice_in_dim(shares, own, 1, axis=1).reshape(n * rows, 1)
    gate = jnp.dot(every, w_gate[0], preferred_element_type=jnp.float32)
    upward = jnp.dot(every, w_up[0], preferred_element_type=jnp.float32)
    hidden = (jax.nn.silu(gate) * upward).astype(jnp.bfloat16)
    partial = jnp.dot(hidden, w_down[0], preferred_element_type=jnp.float32)
    scaled = (partial * share).astype(jnp.bfloat16)
    return lax.psum_scatter(scaled, "ep", scatter_dimension=0, tiled=True)


def solution(mesh):
    in_specs = (
        P(("dp", "ep"), None),
        P(("dp", "ep"), None),
        P(("dp", "ep"), None),
        P("ep", None, None),
        P("ep", None, None),
        P("ep", None, None),
    )
    return jax.shard_map(
        on_device, mesh=mesh, in_specs=in_specs, out_specs=P(("dp", "ep"), None), check_vma=False
    )
```

```python
import collections
import functools

import jax
import jax.numpy as jnp
from jax import lax
from jax.experimental import pallas as pl
from jax.experimental.pallas import tpu as pltpu
from jax.sharding import PartitionSpec as P

LINE = 4
LANES = 128
MESH = pl.DeviceIdType.MESH
VMEM_LIMIT = 62_000_000
GROUPS = 2
CHUNKS = 8
EARLY = (1, 5)
PARTS = 7
BLOCKS = 4
LEAD = 0.5
SLACK = 0.3
FAR = 2
HOP = 2
LATE = 1.4
DOWN = 4
PER = CHUNKS // GROUPS
STEPS = LINE * GROUPS
PIECES = CHUNKS + len(EARLY)
AHEAD = (0,)
END = ((3, 0), (3, 1), (2, 0), (2, 1), (1, 0), (0, 0), (1, 1), (0, 1))
INNER = ((3, 0), (3, 1), (0, 0), (0, 1), (2, 0), (2, 1), (1, 0), (1, 1))


def requantized(tokens):
    rows, width = tokens.shape
    blocks = tokens.astype(jnp.float32).reshape(rows, -1, 16)
    largest = jnp.max(jnp.abs(blocks), axis=2)
    scales = (jnp.maximum(largest, 0.25) / 9.0).astype(jnp.bfloat16).astype(jnp.float32)
    divided = blocks / scales[:, :, None]
    payload = jnp.clip(divided, -6.0, 6.0).astype(jnp.bfloat16).astype(jnp.float32)
    return (payload * scales[:, :, None]).astype(jnp.bfloat16).reshape(rows, width)


def quantize_at(ref):
    rows, width = ref.shape
    many = PARTS
    square = (LANES, LANES)
    source = lax.broadcasted_iota(jnp.int32, square, 0)
    target = lax.broadcasted_iota(jnp.int32, square, 1)
    spread = jnp.where(source == target // 16 * 16 + 15, 1.0, 0.0).astype(ref.dtype)

    def body(i, carry):
        tiles, tops = [], []
        for u in range(many):
            at = pl.ds(pl.multiple_of((i * many + u) * LANES, LANES), LANES)
            values = ref[:, at]
            tiles.append((at, values))
            top = jnp.abs(values)
            for distance in (1, 2, 4, 8):
                top = jnp.maximum(top, pltpu.roll(top, distance, 1))
            tops.append(top)
        largest = jnp.dot(
            jnp.concatenate(tops, axis=0), spread, preferred_element_type=jnp.float32
        )
        results = []
        for u in range(many):
            at, values = tiles[u]
            scales = jnp.maximum(largest[u * rows : (u + 1) * rows], 0.25) / 9.0
            scales = scales.astype(jnp.bfloat16).astype(jnp.float32)
            payload = jnp.clip(values.astype(jnp.float32) / scales, -6.0, 6.0)
            payload = payload.astype(jnp.bfloat16).astype(jnp.float32)
            results.append((payload * scales).astype(ref.dtype))
        for u in range(many):
            ref[:, tiles[u][0]] = results[u]
        return carry

    lax.fori_loop(0, width // LANES // many, body, 0)


def row_of(piece):
    return piece if piece < CHUNKS else EARLY[piece - CHUNKS]


def early_at(z):
    return EARLY if 0 < z < LINE - 1 else EARLY[:FAR]


def in_order():
    return sorted(range(PIECES), key=lambda piece: (row_of(piece) // PER, piece))


def down_line():
    ranks = {piece: rank for rank, piece in enumerate(in_order())}
    ready = {
        z: {(z, piece): max(0, 2 * (piece - CHUNKS) + 2) for piece in range(PIECES)}
        for z in range(LINE)
    }
    sends = {z: [] for z in range(LINE)}
    for slot in range(8 * PIECES):
        for z in range(LINE - 1, 0, -1):
            able = [
                key
                for key, when in ready[z].items()
                if when <= slot and (key[1] < CHUNKS or row_of(key[1]) in early_at(z - 1))
            ]
            if able:
                owner, piece = min(able, key=lambda key: (-key[0], ranks[key[1]]))
                del ready[z][owner, piece]
                sends[z].append((slot, owner, piece))
                if z - 1 > 0:
                    ready[z - 1][owner, piece] = slot + HOP
    return sends


def turn(block):
    early = sorted({c * BLOCKS // CHUNKS for c in EARLY} - set(AHEAD))
    if block in early:
        return 0.1 + early.index(block)
    return block * CHUNKS / BLOCKS - 0.8


def settled(c):
    block = c * BLOCKS // CHUNKS
    return 0 if block in AHEAD else turn(block) + 0.05


def starts(z, moves, arrival):
    latest, found = 0, []
    for number, (slot, owner, piece) in enumerate(moves):
        able = arrival.get((owner, piece), 0)
        if owner == z:
            tail = all(key[1] == z for key in moves[number:])
            able = latest if tail and z in (1, LINE - 2) else max(0, slot - 1)
            able = max(able, settled(row_of(piece)))
            if piece >= CHUNKS:
                able = max(able, 2 * (piece - CHUNKS) + 1.5)
        latest = max(latest, able)
        found.append((latest, owner, piece))
    return found


def flip(order):
    return tuple((LINE - 1 - owner, g) for owner, g in order)


ORDERS = (END, INNER, flip(INNER), flip(END))


FIRST, START = -1, 0
BACK = 4 * 512 / 7168 / GROUPS * CHUNKS / LINE


def before(k):
    return 1 + 3 * k


def middle(k):
    return 2 + 3 * k


def after(k):
    return 3 + 3 * k


LAST = after(STEPS)


def crossings(g, early):
    return [c for c in range(g * PER, g * PER + PER) if c not in early]


def due(k, z):
    total = LEAD + CHUNKS + len(EARLY)
    for o, g in ORDERS[z][: k + 1]:
        total += len(crossings(g, EARLY if o == z else early_at(z))) + BACK
    return total


def ready_at(k, z):
    return due(k, z) + 2


def gap_of(time, least, z):
    k = least
    while k < STEPS - 1 and due(k + 1, z) - SLACK < time:
        k += 1
    return k


def climb(orders):
    down = down_line()
    took = CHUNKS / GROUPS / PARTS
    came = {z: {} for z in range(LINE)}
    adds = {z: [] for z in range(LINE)}
    for z in range(LINE - 1):
        free = max(slot for slot, o, piece in down[LINE - 1 - z]) + 1
        todo = []
        for k in range(STEPS):
            o, g = orders[z][k]
            if o > z:
                for n in range(PARTS):
                    when = ready_at(k, z) + 0.1 * n
                    place = k
                    if z > 0:
                        place = gap_of(came[z][o, g, n], k, z)
                        when = max(came[z][o, g, n], ready_at(place, z))
                    todo.append((place, when, o, g, n))
        for place, when, o, g, n in sorted(todo):
            free = max(free, when) + took
            came[z + 1][o, g, n] = free + 0.3
            adds[z].append((place, when, o, g, n))
    return came, adds


def script(z):
    last = LINE - 1
    down = down_line()
    up = {p: [(slot, last - o, c) for slot, o, c in down[last - p]] for p in range(LINE)}
    arrival = {(z, c): settled(c) for c in range(CHUNKS)}
    if z < last:
        arrival.update({(o, c): slot + LATE for slot, o, c in down[z + 1]})
    if z > 0:
        arrival.update({(o, c): slot + LATE for slot, o, c in up[z - 1]})
    moves = [(slot, "down", o, c) for slot, o, c in starts(z, down[z], arrival)]
    moves += [(slot, "up", o, c) for slot, o, c in starts(z, up[z], arrival)]
    steps = ORDERS[z]
    chunks = [
        [(o, c) for c in crossings(g, EARLY if o == z else early_at(z))] for o, g in steps
    ]
    raw = []

    def add(place, rank, op):
        raw.append((place, rank, len(raw), op))

    begun = {}
    for c in EARLY:
        block = c * BLOCKS // CHUNKS
        begun[c] = 0.5 if block in AHEAD else turn(block) + 0.9
        add(FIRST if block in AHEAD else START, begun[c], ("cross", z, c))
    for slot, way, o, piece in moves:
        if slot == 0 and row_of(piece) * BLOCKS // CHUNKS in AHEAD:
            add(FIRST, 0, ("line", way, o, piece))
        elif slot <= due(0, z) - SLACK:
            add(START, slot, ("line", way, o, piece))
        else:
            k = min(STEPS - 2, gap_of(slot, 0, z))
            place = middle(k) if slot <= due(k, z) + 0.6 else after(k)
            add(place, 1 + slot / 100, ("line", way, o, piece))
    for i in range(BLOCKS):
        if i not in AHEAD:
            add(START, turn(i), ("quantize", i))
    slow = CHUNKS / DOWN
    for i in range(DOWN):
        add(FIRST if i == 0 else START, max(1, max(begun.values()) + 0.01), ("weights", i))
        add(START, len(EARLY) + (i + 1) * slow + 0.6, ("weights y", i))
        when = len(EARLY) + (i + 2) * slow + 1.1
        add(START if when < due(0, z) else before(0), when, ("weights x", i))
    latest = 0
    for o, c in chunks[0] + chunks[1][:1]:
        latest = max(latest, arrival[o, c] + 0.2)
        add(START, latest, ("cross", o, c))
    for k in range(STEPS):
        o, g = steps[k]
        for c in range(g * PER, g * PER + PER):
            add(before(k), 0, ("arrived", o, c))
            if o != z and c in early_at(z):
                add(before(k), 0.5, ("arrived", o, CHUNKS + EARLY.index(c)))
            else:
                add(before(k), 1, ("crossed", o, c))
            add(middle(k), 2, ("free", o, c))
        if k + 1 < STEPS:
            for o, c in chunks[k + 1][1:]:
                add(middle(k), 0, ("cross", o, c))
        if k + 2 < STEPS:
            add(after(k), -1, ("cross",) + chunks[k + 2][0])
    flipped = [flip(ORDERS[last - p]) for p in range(LINE)]
    came_up, adds_up = climb(ORDERS)
    came_down, adds_down = climb(flipped)
    came, adds = {}, []
    if z > 0:
        for key, when in came_up[z].items():
            came[key] = max(came.get(key, 0), when)
        if z < last:
            adds += adds_up[z]
    if z < last:
        for (o, g, n), when in came_down[last - z].items():
            came[last - o, g, n] = max(came.get((last - o, g, n), 0), when)
        if z > 0:
            adds += [(k, when, last - o, g, n) for k, when, o, g, n in adds_down[last - z]]
    for k, when, o, g, n in sorted(adds):
        add(after(k), when, ("add", o, g, n))
    for g in range(GROUPS):
        for n in range(PARTS):
            k = STEPS - 1
            add(after(k), max(came[z, g, n], ready_at(k, z)), ("finish", z, g, n))
    waited, sent, freed = set(), [], set()
    done = collections.defaultdict(list)
    for place, rank, number, op in sorted(raw):
        out = done[place]
        kind, key = op[0], op[-2:]
        if kind in ("add", "finish"):
            if out and out[-1][:3] == op[:3] and out[-1][4] == op[3]:
                out[-1] = out[-1][:4] + (op[3] + 1,)
            else:
                out.append(op + (op[3] + 1,))
            continue
        if kind in ("line", "cross", "arrived") and key not in waited:
            if key[0] != z:
                waited.add(key)
                out.append(("wait",) + key)
            elif key[1] >= CHUNKS:
                waited.add(key)
                out.append(("crossed", z, EARLY[key[1] - CHUNKS]))
        if kind == "crossed":
            early = EARLY.index(key[1]) + CHUNKS if key[1] in EARLY else None
            if early is not None and key[0] == z:
                if (z, early) not in waited:
                    waited.add((z, early))
                    out.append(op)
                continue
        if kind == "arrived":
            continue
        if kind in ("line", "cross"):
            assert key not in freed
            sent.append((op[1] if kind == "line" else "cross",) + key)
        if kind == "free":
            freed.add(key)
            for item in list(sent):
                if item[1:] == key:
                    sent.remove(item)
                    out.append(("sent",) + item)
            continue
        out.append(op)
    assert len(freed) == LINE * CHUNKS
    for item in sent:
        done[LAST].append(("sent",) + item)
    return done


def layer(
    tokens_ref,
    ids_ref,
    affinity_ref,
    gate_ref,
    up_ref,
    down_ref,
    result_ref,
    out_ref,
    x_ref,
    wg_ref,
    wu_ref,
    wd_ref,
    hid_ref,
    peer_ref,
    got_ref,
    shares_ref,
    local,
    line_send,
    line_recv,
    cross_send,
    cross_recv,
    hid_send,
    hid_recv,
    part_send,
    part_recv,
    share_send,
    share_recv,
    w_send,
    w_recv,
):
    me, dp = lax.axis_index("ep"), lax.axis_index("dp")
    here, y = me // 2, lax.rem(me, 2)
    other = 1 - y
    last = LINE - 1
    peer = {"ep": 2 * here + other}
    twin = {"dp": dp + 1 - 2 * lax.rem(dp, 2)}
    across = {"dp": lax.rem(dp + 2, 4)}
    rows, width = out_ref.shape
    lot = rows // GROUPS
    size = rows // CHUNKS
    part = width // PARTS
    inner = wg_ref.shape[1]
    scripts = [script(z) for z in range(LINE)]

    def chunk(o, c):
        g, i = c // PER, c % PER
        return x_ref.at[o, g, pl.ds(pl.multiple_of(y * lot + i * size, size), size), :]

    def crossing(o, c):
        g, i = c // PER, c % PER
        return x_ref.at[o, g, pl.ds(pl.multiple_of(other * lot + i * size, size), size), :]

    def remote(source, place, send, recv, target):
        return pltpu.make_async_remote_copy(
            src_ref=source,
            dst_ref=place,
            send_sem=send,
            recv_sem=recv,
            device_id=target,
            device_id_type=MESH,
        )

    def line(way, o, c):
        target = {"ep": me + 2 if way == "up" else me - 2}
        place = chunk(o, c) if c < CHUNKS else crossing(o, EARLY[c - CHUNKS])
        return remote(
            place, place, line_send.at[0 if way == "up" else 1, o, c], line_recv.at[o, c], target
        )

    def cross(o, c):
        place = chunk(o, c)
        return remote(place, place, cross_send.at[o, c], cross_recv.at[o, c], peer)

    quarter = down_ref.shape[1] // 4
    piece = quarter // DOWN

    def rows_of(q, i):
        return pl.ds(pl.multiple_of(q * quarter + i * piece, piece), piece)

    def weight(kind, half, q, i, target):
        place = wd_ref.at[half, rows_of(q, i), :]
        source = down_ref.at[0, rows_of(q, i), :] if kind == 0 else place
        return remote(source, place, w_send.at[kind], w_recv.at[kind, i], target)

    q_mine, q_across = dp, lax.rem(dp + 2, 4)
    twin_dp = dp + 1 - 2 * lax.rem(dp, 2)
    q_twin, q_twin_across = twin_dp, lax.rem(twin_dp + 2, 4)

    def partial(z, o, g, n, way):
        step = 1 if way == "up" else -1
        nearest = isinstance(z, int) and z + step == o
        slot = LINE if way == "down" and nearest else o
        return part_copy(o, slot, g, n, {"ep": me + 2 * step})

    def part_copy(o, slot, g, n, target):
        columns = pl.ds(pl.multiple_of(n * part, part), part)
        source = x_ref.at[o, g, pl.ds(pl.multiple_of(y * lot, lot), lot), columns]
        return remote(
            source,
            got_ref.at[slot, g, :, columns],
            part_send.at[o, g],
            part_recv.at[slot, g, n],
            target,
        )

    def got_wait(slot, g, n):
        columns = pl.ds(pl.multiple_of(n * part, part), part)
        place = got_ref.at[slot, g, :, columns]
        remote(place, place, part_send.at[0, g], part_recv.at[slot, g, n], peer).wait_recv()

    def sum_into(target, at, sources):
        step = 16

        def body(i, carry):
            lines = pl.ds(pl.multiple_of(i * step, step), step)
            total = sources[0][lines, at].astype(jnp.float32)
            for source in sources[1:]:
                total = total + source[lines, at].astype(jnp.float32)
            target[lines, at] = total.astype(target.dtype)
            return carry

        lax.fori_loop(0, lot // step, body, 0)

    def quantize(i):
        block = rows // BLOCKS
        g, at = i * block // lot, i * block % lot
        lines = pl.ds(pl.multiple_of(y * lot + at, block), block)
        quantize_at(x_ref.at[here, g, lines, :])

    def run(z, op):
        kind = op[0]
        if kind == "wait":
            line("up", *op[1:]).wait_recv()
        elif kind == "line":
            line(*op[1:]).start()
        elif kind == "cross":
            cross(*op[1:]).start()
        elif kind == "crossed":
            place = crossing(*op[1:])
            o, c = op[1:]
            remote(place, place, cross_send.at[o, c], cross_recv.at[o, c], peer).wait_recv()
        elif kind == "sent":
            way, o, c = op[1:]
            (cross(o, c) if way == "cross" else line(way, o, c)).wait_send()
        elif kind == "quantize":
            quantize(op[1])
        elif kind == "weights":
            weight(0, y, q_mine, op[1], peer).start()
        elif kind == "weights y":
            weight(0, other, q_mine, op[1], peer).wait_recv()
            weight(1, other, q_mine, op[1], across).start()
            weight(2, other, q_mine, op[1], twin).start()
        elif kind == "weights x":
            weight(1, other, q_across, op[1], across).wait_recv()
            weight(3, other, q_across, op[1], twin).start()
        elif kind == "add":
            o, g, begin, end = op[1:]
            mine = x_ref.at[o, g, pl.ds(pl.multiple_of(y * lot, lot), lot), :]

            def body(n, carry):
                got_wait(o, g, n)
                at = pl.ds(pl.multiple_of(n * part, part), part)
                sum_into(mine, at, [mine, got_ref.at[o, g]])
                partial(z, o, g, n, "up" if o > z else "down").start()
                return carry

            lax.fori_loop(begin, end, body, 0)
        elif kind == "finish":
            g, begin, end = op[2:]
            mine = x_ref.at[z, g, pl.ds(pl.multiple_of(y * lot, lot), lot), :]
            slots = ([z] if z > 0 else []) + ([LINE] if z < last else [])

            def body(n, carry):
                for slot in slots:
                    got_wait(slot, g, n)
                at = pl.ds(pl.multiple_of(n * part, part), part)
                sum_into(
                    out_ref.at[pl.ds(g * lot, lot), :],
                    at,
                    [mine] + [got_ref.at[slot, g] for slot in slots],
                )
                place = pl.ds(g * lot, lot)
                pltpu.make_async_copy(
                    out_ref.at[place, at], result_ref.at[place, at], local.at[GROUPS + 3]
                ).start()
                return carry

            lax.fori_loop(begin, end, body, 0)
        else:
            raise ValueError(kind)

    def play(place):
        for z in range(LINE):
            ops = scripts[z][place]
            if ops:

                @pl.when(here == z)
                def _(z=z, ops=ops):
                    for op in ops:
                        run(z, op)

    def play_in(kind, k):
        for z in range(LINE):

            @pl.when(here == z)
            def _(z=z):
                for step in range(STEPS):
                    ops = scripts[z][kind(step)]
                    if ops:

                        @pl.when(k == step)
                        def _(ops=ops):
                            for op in ops:
                                run(z, op)

    own_rows = pl.ds(pl.multiple_of(y * lot, lot), lot)
    loads = []

    def load(source, place):
        copy = pltpu.make_async_copy(source, place, local.at[len(loads)])
        loads.append(copy)
        copy.start()

    for g in range(GROUPS):
        load(tokens_ref.at[pl.ds(g * lot, lot), :], x_ref.at[here, g, own_rows, :])
    barrier = pltpu.get_barrier_semaphore()
    targets = [{"ep": lax.rem(me + 2 * step, 2 * LINE)} for step in range(1, LINE)]
    targets += [peer, twin, across]
    for target in targets:
        pl.semaphore_signal(barrier, inc=1, device_id=target, device_id_type=MESH)

    loads[0].wait()
    choices = ids_ref.shape[0]
    names = lax.broadcasted_iota(jnp.int32, shares_ref.shape[1:], 0)
    whole = sum(affinity_ref[i : i + 1, :] for i in range(choices))
    shares_ref[here] = sum(
        jnp.where(ids_ref[i : i + 1, :] == names, affinity_ref[i : i + 1, :] / whole, 0.0)
        for i in range(choices)
    )
    for i in AHEAD:
        quantize(i)
    pl.semaphore_wait(barrier, len(targets))
    play(FIRST)
    load(gate_ref.at[0], wg_ref)
    load(up_ref.at[0], wu_ref)
    load(down_ref.at[0], wd_ref.at[y])
    for copy in loads[1:GROUPS]:
        copy.wait()
    shares = []
    for step in range(1, LINE):
        target = {"ep": lax.rem(me + 2 * step, 2 * LINE)}
        mine = shares_ref.at[here]
        copy = remote(mine, mine, share_send.at[step], share_recv.at[step], target)
        copy.start()
        shares.append(copy)
    play(START)
    for copy in loads[GROUPS:]:
        copy.wait()
    for copy in shares:
        copy.wait()

    def order(k, which):
        value = jnp.int32(0)
        for z in range(LINE):
            for i in range(STEPS):
                if ORDERS[z][i][which]:
                    value = jnp.where((here == z) & (k == i), ORDERS[z][i][which], value)
        return value

    half = inner // 2

    def step_of(k, carry):
        o, g = order(k, 0), order(k, 1)
        play_in(before, k)

        def hidden(j, c):
            at = pl.ds(pl.multiple_of(j * half, half), half)
            x = x_ref[o, g]
            gate = jnp.dot(x, wg_ref[:, at], preferred_element_type=jnp.float32)
            upward = jnp.dot(x, wu_ref[:, at], preferred_element_type=jnp.float32)
            hid_ref[o, g, :, at] = (jax.nn.silu(gate) * upward).astype(hid_ref.dtype)
            return c

        lax.fori_loop(0, 2, hidden, 0)
        other_rows = pl.ds(pl.multiple_of(other * lot, lot), lot)
        back = remote(
            hid_ref.at[o, g, other_rows, :],
            peer_ref.at[o, g],
            hid_send.at[o, g],
            hid_recv.at[o, g],
            peer,
        )
        back.start()
        play_in(middle, k)

        @pl.when(k == 0)
        def _():
            for i in range(DOWN):
                weight(2, other, q_twin, i, twin).wait_recv()
                weight(3, other, q_twin_across, i, twin).wait_recv()

        back.wait()
        row = shares_ref[o, pl.ds(here, 1), :]
        square = (lot, row.shape[1])
        lane = lax.broadcasted_iota(jnp.int32, square, 1)
        line_of = lax.broadcasted_iota(jnp.int32, square, 0)
        share = jnp.sum(
            jnp.where(lane == line_of + g * lot, jnp.broadcast_to(row, square), 0.0),
            axis=1,
            keepdims=True,
        )
        begins = ((here == 0) & (o != 0)) | ((here == last) & (o != last))
        slot = jnp.where((here == last) & (o == last - 1), LINE, o)
        onward = jnp.where(here == 0, me + 2, me - 2)

        def down(n, c):
            at = pl.ds(pl.multiple_of(n * part, part), part)
            total = jnp.dot(
                hid_ref[o, g, own_rows, :], wd_ref[y, :, at], preferred_element_type=jnp.float32
            ) + jnp.dot(peer_ref[o, g], wd_ref[other, :, at], preferred_element_type=jnp.float32)
            x_ref[o, g, own_rows, at] = (total * share).astype(x_ref.dtype)

            @pl.when(begins)
            def _():
                part_copy(o, slot, g, n, {"ep": onward}).start()

            return c

        lax.fori_loop(0, PARTS, down, 0)
        play_in(after, k)
        return carry

    lax.fori_loop(0, STEPS, step_of, 0)

    def drain(i, carry):
        o, g = i // GROUPS, lax.rem(i, GROUPS)

        @pl.when(o != here)
        def _():
            whole = x_ref.at[o, g, own_rows, :]
            remote(whole, whole, part_send.at[o, g], part_recv.at[o, g, 0], peer).wait_send()

        return carry

    lax.fori_loop(0, STEPS, drain, 0)
    play(LAST)
    pltpu.make_async_copy(out_ref, result_ref, local.at[GROUPS + 3]).wait()
    for kind in range(4):
        whole = wd_ref.at[0, pl.ds(0, quarter), :]
        remote(whole, whole, w_send.at[kind], w_recv.at[kind, 0], peer).wait_send()


def fused(tokens, expert_ids, affinity, w_gate, w_up, w_down):
    rows, width = tokens.shape
    inner = w_gate.shape[2]
    lot = rows // GROUPS
    kind = tokens.dtype
    dma = pltpu.SemaphoreType.DMA
    anywhere = pl.BlockSpec(memory_space=pl.ANY)
    inside = pl.BlockSpec(memory_space=pltpu.VMEM)
    return pl.pallas_call(
        layer,
        out_shape=jax.ShapeDtypeStruct((rows, width), kind),
        in_specs=[anywhere, inside, inside, anywhere, anywhere, anywhere],
        out_specs=anywhere,
        scratch_shapes=[
            pltpu.VMEM((rows, width), kind),
            pltpu.VMEM((LINE, GROUPS, 2 * lot, width), kind),
            pltpu.VMEM((width, inner), kind),
            pltpu.VMEM((width, inner), kind),
            pltpu.VMEM((2, inner, width), kind),
            pltpu.VMEM((LINE, GROUPS, 2 * lot, inner), kind),
            pltpu.VMEM((LINE, GROUPS, lot, inner), kind),
            pltpu.VMEM((LINE + 1, GROUPS, lot, width), kind),
            pltpu.VMEM((LINE, 8, rows), affinity.dtype),
            dma((GROUPS + 4,)),
            dma((2, LINE, PIECES)),
            dma((LINE, PIECES)),
            dma((LINE, CHUNKS)),
            dma((LINE, CHUNKS)),
            dma((LINE, GROUPS)),
            dma((LINE, GROUPS)),
            dma((LINE, GROUPS)),
            dma((LINE + 1, GROUPS, PARTS)),
            dma((LINE,)),
            dma((LINE,)),
            dma((4,)),
            dma((4, DOWN)),
        ],
        compiler_params=pltpu.CompilerParams(
            collective_id=0, has_side_effects=True, vmem_limit_bytes=VMEM_LIMIT
        ),
        name="layer",
    )(tokens, expert_ids.T, affinity.T, w_gate, w_up, w_down)


def on_device(tokens, expert_ids, affinity, w_gate, w_up, w_down):
    n = lax.axis_size("ep")
    experts = n // 2
    own = lax.axis_index("ep") // 2
    rows, width = tokens.shape
    by_line = (
        experts == LINE
        and lax.axis_size("dp") == 4
        and rows == LANES
        and width % (PARTS * LANES) == 0
    )
    if by_line:
        return fused(tokens, expert_ids, affinity, w_gate, w_up, w_down)
    weights = affinity / jnp.sum(affinity, axis=1, keepdims=True)
    padded = -(-experts // 8) * 8
    names = jnp.arange(padded, dtype=jnp.int32)[:, None]
    shares = sum(
        jnp.where(expert_ids[:, k][None, :] == names, weights[:, k][None, :], 0.0)
        for k in range(weights.shape[1])
    )
    every = lax.all_gather(requantized(tokens), "ep", axis=0, tiled=False)
    shares = lax.all_gather(shares, "ep", axis=0, tiled=False)
    every = every.reshape(n * rows, width)
    share = lax.dynamic_slice_in_dim(shares, own, 1, axis=1).reshape(n * rows, 1)
    gate = jnp.dot(every, w_gate[0], preferred_element_type=jnp.float32)
    upward = jnp.dot(every, w_up[0], preferred_element_type=jnp.float32)
    hidden = (jax.nn.silu(gate) * upward).astype(jnp.bfloat16)
    partial = jnp.dot(hidden, w_down[0], preferred_element_type=jnp.float32)
    scaled = (partial * share).astype(jnp.bfloat16)
    return lax.psum_scatter(scaled, "ep", scatter_dimension=0, tiled=True)


def solution(mesh):
    in_specs = (
        P(("dp", "ep"), None),
        P(("dp", "ep"), None),
        P(("dp", "ep"), None),
        P("ep", None, None),
        P("ep", None, None),
        P("ep", None, None),
    )
    return jax.shard_map(
        on_device, mesh=mesh, in_specs=in_specs, out_specs=P(("dp", "ep"), None), check_vma=False
    )
```
